512 devices in a mesh: blk: 32 (over x, y), grp: 16 (over z, core).
Axes of the slice: x: 4, y: 8, z: 8, core: 2. Of those that a mesh axis runs over, the one named last changes fastest.
Arguments:
- queries: bfloat16 [192, 8192], P(None, ('blk', 'grp')), may hold values from -6 to 6
- key_pool: bfloat16 [16, 256, 128, 1024], P('grp', 'blk'), may hold values from -28 to 28
- value_pool: bfloat16 [16, 256, 128, 1024], P('grp', 'blk'), may hold values from -6 to 6
- lengths: int32 [16, 4], P('grp'), may hold values from 1 to 128, as said below
- block_table: int32 [16, 4, 128], P('grp'), may hold values from 0 to 255, as said below
Outputs:
- attended: bfloat16 [192, 8192], P('grp', 'blk')
The draws below stay inside these ranges and needn't reach their ends.
Inputs may be any that keep to these rules, and one draw needn't show every extreme that they name: Each group's 4 lengths add up to 208, and one of them is exactly 128. Within a group, the entries block_table[g, q, j] with j < lengths[g, q] are distinct slots; entries past a sequence's length are arbitrary slots and unused. Slots s * 8 to s * 8 + 7 form the s-th aligned block of the pool; at least 4 and at most 8 live slots lie in one aligned block, and exactly 8 in some aligned block of every group.
All inputs are finite; a program needn't handle non-finite values.
Results may differ from the reference program's by a relative error of at most 0.0049.
Values may be sent and summed in bfloat16 or wider, within the bound.
No kernel may reach another device: no remote copies, remote signals or barrier semaphores. Data moves between devices by JAX's collectives and lax.ppermute only.
A program may use at most 64 MiB of HBM per device.

```python
import math
import jax
import jax.numpy as jnp
from jax import lax

HQ = 64
KVH = 8
DH = 128
BLOCK = 128
STEPS = 3
Q_DEV = 4
SLOTS = 8
GROUPS = 16
QUERIES = 64
POOL = 256
MAXB = 128
N_BLK = 32


def group_layout(group_key):
    subkeys = jax.random.split(group_key, 9)
    patterns = jnp.array([[8, 8, 6, 4], [8, 6, 6, 6], [7, 7, 6, 6], [8, 7, 7, 4], [8, 8, 5, 5], [7, 7, 8, 4], [8, 6, 7, 5]], jnp.int32)
    quartets = N_BLK // 4
    chosen = jax.random.randint(subkeys[0], (quartets,), 0, 7)
    forced = jnp.array([0, 3, 4], jnp.int32)[jax.random.randint(subkeys[1], (), 0, 3)]
    chosen = chosen.at[0].set(forced)
    device_loads = patterns[chosen].reshape(N_BLK)
    device_loads = device_loads[jax.random.permutation(subkeys[2], N_BLK)]
    slot_ranks = jax.vmap(lambda sub: jax.random.permutation(sub, SLOTS))(jax.random.split(subkeys[3], N_BLK))
    live = (slot_ranks < device_loads[:, None]).reshape(POOL)
    shuffle = jax.random.permutation(subkeys[4], POOL).astype(jnp.int32)
    sort_key = jnp.where(live, shuffle, POOL + shuffle)
    slot_list = jnp.argsort(sort_key, stable=True).astype(jnp.int32)
    longest = MAXB
    rest = 13 * N_BLK // 2 - longest
    first_part = jax.random.randint(subkeys[5], (), 1, rest - 1)
    second_part = jax.random.randint(subkeys[6], (), 1, rest - first_part)
    third_part = rest - first_part - second_part
    pieces = jnp.stack([jnp.array(longest, jnp.int32), first_part, second_part, third_part]).astype(jnp.int32)
    seq_lengths = pieces[jax.random.permutation(subkeys[7], 4)]
    starts = jnp.cumsum(seq_lengths) - seq_lengths
    block_ids = jnp.arange(MAXB, dtype=jnp.int32)
    where_index = jnp.minimum(starts[:, None] + block_ids[None, :], POOL - 1)
    filler = jax.random.randint(subkeys[8], (Q_DEV, MAXB), 0, POOL)
    slot_table = jnp.where(block_ids[None, :] < seq_lengths[:, None], slot_list[where_index], filler)
    return (seq_lengths.astype(jnp.int32), slot_table.astype(jnp.int32))


def layout_all(key):
    group_keys = jax.random.split(jax.random.fold_in(key, 11), GROUPS)
    return jax.vmap(group_layout)(group_keys)


def query_values(key):
    subkey = jax.random.fold_in(key, 23)
    drawn = jnp.clip(jax.random.normal(subkey, (QUERIES * STEPS, HQ * DH), jnp.float32), -6.0, 6.0)
    return drawn


def draw_queries(key, part):
    return query_values(key).astype(jnp.bfloat16)


def draw_lengths(key, part):
    return layout_all(key)[0]


def draw_block_table(key, part):
    return layout_all(key)[1]


def draw_key_pool(key, part):
    subkey = jax.random.fold_in(key, 31)
    pool_shape = (GROUPS, POOL, BLOCK, KVH * DH)
    drawn = jnp.clip(jax.random.normal(subkey, pool_shape, jnp.float32), -6.0, 6.0)
    return drawn.astype(jnp.bfloat16)


def level_of(rng, extent, cuts, smallest, top_value):
    loudness = 1.0
    for dim, blocks in cuts:
        heights = jax.random.uniform(jax.random.fold_in(jax.random.fold_in(rng, 6), dim), (blocks,), jnp.float32, smallest / len(cuts), top_value / len(cuts))
        loudness = loudness * jnp.repeat(jnp.exp(heights), extent[dim] // blocks).reshape((-1,) + (1,) * (len(extent) - 1 - dim))
    return loudness


def scatter_about(stream_key, shape, spread, most, cuts=(), kind=jnp.bfloat16):
    loudness = level_of(stream_key, shape, cuts, -0.22, 0.18) if cuts else 1.0
    entries = jax.random.normal(stream_key, shape, jnp.float32) * spread * loudness
    return jnp.minimum(jnp.maximum(entries, -most), most).astype(kind)


def setup_inputs(seed: int = 0) -> dict:
    key_list = jax.random.split(jax.random.key(seed), 6)
    return {
        "queries": draw_queries(jax.random.fold_in(key_list[5], 71), 0),
        "key_pool": draw_key_pool(jax.random.fold_in(key_list[5], 71), 0),
        "value_pool": scatter_about(key_list[2], (GROUPS, POOL, BLOCK, KVH * DH), 1.0, 6.0, ((0, 16), (1, 32))),
        "lengths": draw_lengths(jax.random.fold_in(key_list[5], 71), 0),
        "block_table": draw_block_table(jax.random.fold_in(key_list[5], 71), 0),
    }


empty_max = -1e+30

def owners(seq_lengths, slot_table, first_slot, slot_count):
    slot_ids = first_slot + jnp.arange(slot_count, dtype=jnp.int32)
    places = jnp.arange(slot_table.shape[1], dtype=jnp.int32)
    in_length = places[None, :] < seq_lengths[:, None]
    matches = (slot_table[:, :, None] == slot_ids[None, None, :]) & in_length[:, :, None]
    return jnp.transpose(jnp.any(matches, axis=1))

def slot_partials(query_block, key_block, value_block):
    slot_count = key_block.shape[0]
    per_group = HQ // KVH
    grouped_q = query_block.reshape(slot_count, STEPS, KVH, per_group, DH)
    grouped_q = jnp.transpose(grouped_q, (0, 2, 1, 3, 4)).reshape(slot_count, KVH, STEPS * per_group, DH).astype(jnp.float32)
    key_heads = key_block.reshape(slot_count, key_block.shape[1], KVH, DH).astype(jnp.float32)
    value_heads = value_block.reshape(slot_count, value_block.shape[1], KVH, DH).astype(jnp.float32)
    scores = jnp.einsum('cgqd,ctgd->cgqt', grouped_q, key_heads) * (1.0 / math.sqrt(DH))
    block_max = lax.optimization_barrier(jnp.max(scores, axis=3))
    weights = jnp.exp(scores - block_max[..., None]).astype(jnp.bfloat16)
    block_total = lax.optimization_barrier(jnp.sum(weights.astype(jnp.float32), axis=3))
    block_out = jnp.einsum('cgqt,ctgd->cgqd', weights.astype(jnp.float32), value_heads)
    return (block_max, block_total, block_out)

def gather_sequences(owned, block_max, block_total, block_out):
    masked = jnp.where(owned[:, :, None, None], block_max[:, None], empty_max)
    seq_max = lax.optimization_barrier(jnp.max(masked, axis=0))
    factor = jnp.where(owned[:, :, None, None], jnp.exp(block_max[:, None] - seq_max[None]), 0.0)
    seq_total = lax.optimization_barrier(jnp.sum(factor * block_total[:, None], axis=0))
    seq_out = jnp.einsum('cqgh,cghd->qghd', factor, block_out, precision=lax.Precision.HIGHEST)
    seq_count = owned.shape[1]
    per_group = HQ // KVH
    seq_max = jnp.transpose(seq_max.reshape(seq_count, KVH, STEPS, per_group), (0, 2, 1, 3)).reshape(seq_count * STEPS, HQ)
    seq_total = jnp.transpose(seq_total.reshape(seq_count, KVH, STEPS, per_group), (0, 2, 1, 3)).reshape(seq_count * STEPS, HQ)
    seq_out = jnp.transpose(seq_out.reshape(seq_count, KVH, STEPS, per_group, DH), (0, 2, 1, 3, 4)).reshape(seq_count * STEPS, HQ, DH)
    return (seq_max, seq_total, seq_out)

def reference(queries, key_pool, value_pool, lengths, block_table):
    grouped = queries.reshape(GROUPS, Q_DEV, STEPS * HQ * DH)

    def one_group(inputs):
        seq_rows, key_rows, value_rows, seq_lengths, slot_table = inputs
        owned = owners(seq_lengths, slot_table, 0, POOL)
        query_block = jnp.dot(owned.astype(jnp.float32), seq_rows.astype(jnp.float32), precision=lax.Precision.HIGHEST).astype(jnp.bfloat16)
        block_max, block_total, block_out = slot_partials(query_block, key_rows, value_rows)
        seq_max, seq_total, seq_out = gather_sequences(owned, block_max, block_total, block_out)
        return (seq_out / seq_total[..., None]).astype(jnp.bfloat16).reshape(Q_DEV * STEPS, HQ * DH)
    attended = lax.map(one_group, (grouped, key_pool, value_pool, lengths, block_table))
    return attended.reshape(QUERIES * STEPS, HQ * DH)
```

```python
import math

import jax
import jax.numpy as jnp
from jax import lax
from jax.experimental import pallas as pl
from jax.experimental.pallas import tpu as pltpu
from jax.sharding import PartitionSpec as P

HQ = 64
KVH = 8
DH = 128
STEPS = 3
SEQS = 4
TOK = SEQS * STEPS
HEADS = 2
ROWS = HEADS * TOK
SLICES = 4
SLOTS = 8
BLOCK = 128
LANES = 128
SCALE = math.log2(math.e) / math.sqrt(DH)
LN2 = math.log(2.0)
EMPTY = -1e30

VMEM = pl.BlockSpec(memory_space=pltpu.VMEM)
SMEM = pl.BlockSpec(memory_space=pltpu.SMEM)


def iota(shape, dim):
    return lax.broadcasted_iota(jnp.int32, shape, dim)


def pack_kernel(q_ref, out_ref):
    groups, feats, _ = out_ref.shape
    q = q_ref[...].astype(jnp.float32)
    keep = iota((feats, LANES), 1) < TOK
    wide = jnp.concatenate([q, jnp.zeros((feats, 2 * LANES - q.shape[1]), jnp.float32)], axis=1)
    for g in range(groups):
        at = g * TOK
        shifted = wide if at == 0 else pltpu.roll(wide, 2 * LANES - at, 1)
        out_ref[g] = jnp.where(keep, shifted[:, :LANES], 0.0).astype(out_ref.dtype)


def spread_kernel(a_ref, out_ref):
    row = iota((ROWS, LANES), 0)
    tok = jnp.where(row >= TOK, row - TOK, row)
    pick = (tok == iota((ROWS, LANES), 1)).astype(jnp.bfloat16)
    nt = (((1,), (1,)), ((), ()))
    first = lax.dot_general(pick, a_ref[:LANES, :], nt, preferred_element_type=jnp.float32)
    second = lax.dot_general(pick, a_ref[LANES:, :], nt, preferred_element_type=jnp.float32)
    rows = jnp.where(row < TOK, first, second).astype(out_ref.dtype)
    for b in range(out_ref.shape[0]):
        out_ref[b] = rows


def attend_kernel(first_ref, len_ref, table_ref, q_ref, k_ref, v_ref, out_ref):
    lane4 = iota((SEQS, LANES), 1)
    sub4 = iota((SEQS, LANES), 0)
    lens = jnp.zeros((SEQS, LANES), jnp.int32)
    for q in range(SEQS):
        lens = jnp.where(sub4 == q, len_ref[0, q], lens)
    local = jnp.where(lane4 < lens, table_ref[...] - first_ref[0], -1)
    row = iota((ROWS, LANES), 0)
    seq = jnp.where(row >= TOK, row - TOK, row) // STEPS
    bias = []
    for s in range(SLOTS):
        hit = jnp.max((local == s).astype(jnp.float32), axis=1, keepdims=True)
        off = jnp.broadcast_to(jnp.where(hit > 0.0, 0.0, EMPTY), (SEQS, LANES))
        b = jnp.broadcast_to(off[0:1], (ROWS, LANES))
        for q in range(1, SEQS):
            b = jnp.where(seq == q, off[q : q + 1], b)
        bias.append(b)
    bias = jnp.concatenate(bias, axis=1)
    bias = jnp.concatenate([bias] * SLICES, axis=0)

    rows = SLICES * ROWS
    lane = iota((rows, LANES), 1)
    lse = jnp.zeros((rows, LANES), jnp.float32)
    nt = (((1,), (1,)), ((), ()))
    nn = (((1,), (0,)), ((), ()))
    for k in range(KVH):
        cols = slice(k * DH, (k + 1) * DH)
        qk = q_ref[k * SLICES : (k + 1) * SLICES].reshape(rows, DH)
        s = lax.dot_general(qk, k_ref[:, cols], nt, preferred_element_type=jnp.float32) + bias
        top = jnp.max(s, axis=1, keepdims=True)
        p = jnp.exp2((s - top) * SCALE).astype(jnp.bfloat16)
        total = jnp.sum(p.astype(jnp.float32), axis=1, keepdims=True)
        o = lax.dot_general(p, v_ref[:, cols], nn, preferred_element_type=jnp.float32)
        o = (o / total).astype(out_ref.dtype)
        lse = jnp.where(lane == k, top * SCALE + jnp.log2(total), lse)
        out_ref[k * SLICES : (k + 1) * SLICES, :ROWS, :] = o.reshape(SLICES, ROWS, DH)
    square = jnp.concatenate([lse, jnp.zeros((LANES - rows, LANES), jnp.float32)], axis=0)
    flat = jnp.transpose(square)[:KVH]
    lane8 = iota((KVH, LANES), 1)
    for j in range(SLICES):
        mine = flat if j == 0 else pltpu.roll(flat, LANES - j * ROWS, 1)
        mine = jnp.where(lane8 < ROWS, mine, 0.0)
        high = mine.astype(jnp.bfloat16).astype(jnp.float32)
        rest = mine - high
        mid = rest.astype(jnp.bfloat16).astype(jnp.float32)
        low = rest - mid
        line = high + pltpu.roll(mid, 32, 1) + pltpu.roll(low, 64, 1)
        for k in range(KVH):
            tile = jnp.broadcast_to(line[k : k + 1], (8, LANES))
            out_ref[k * SLICES + j, ROWS:, :] = tile.astype(out_ref.dtype)


def combine_kernel(a_ref, out_ref):
    devices = a_ref.shape[0]
    sub8 = iota((8, LANES), 0)
    parts = []
    for t in range(devices // 8):
        acc = a_ref[8 * t, ROWS:, :].astype(jnp.float32)
        for j in range(1, 8):
            acc = jnp.where(sub8 == j, a_ref[8 * t + j, ROWS:, :].astype(jnp.float32), acc)
        parts.append(acc)
    stat = jnp.concatenate(parts, axis=0)
    lse = stat + pltpu.roll(stat, LANES - 32, 1) + pltpu.roll(stat, LANES - 64, 1)
    top = jnp.max(lse, axis=0, keepdims=True)
    w = jnp.exp2(lse - top)
    w = w / jnp.sum(w, axis=0, keepdims=True)
    square = jnp.concatenate([w, jnp.zeros((LANES - devices, LANES), jnp.float32)], axis=0)
    wt = jnp.transpose(square)[:ROWS]
    acc = jnp.zeros((ROWS, LANES), jnp.float32)
    for b in range(devices):
        acc = acc + wt[:, b : b + 1] * a_ref[b, :ROWS, :].astype(jnp.float32)
    out_ref[...] = jnp.concatenate([acc[:TOK], acc[TOK:]], axis=1).astype(out_ref.dtype)


def body(queries, key_pool, value_pool, lengths, block_table):
    bf16 = jnp.bfloat16
    groups = lax.axis_size("grp")
    devices = lax.axis_size("blk")
    feats = queries.shape[1]
    packed = pl.pallas_call(
        pack_kernel,
        out_shape=jax.ShapeDtypeStruct((groups, feats, LANES), bf16),
        in_specs=[VMEM],
        out_specs=VMEM,
        name="pack",
    )(queries.T)
    arrived = lax.all_to_all(packed, "grp", split_axis=0, concat_axis=0, tiled=True)
    spread = pl.pallas_call(
        spread_kernel,
        out_shape=jax.ShapeDtypeStruct((devices, ROWS, LANES), bf16),
        in_specs=[VMEM],
        out_specs=VMEM,
        name="spread",
    )(arrived.reshape(groups * feats, LANES))
    query_all = lax.all_to_all(spread, "blk", split_axis=0, concat_axis=0, tiled=True)
    first = (lax.axis_index("blk") * SLOTS).astype(jnp.int32).reshape(1)
    partial = pl.pallas_call(
        attend_kernel,
        out_shape=jax.ShapeDtypeStruct((devices, ROWS + 8, LANES), bf16),
        in_specs=[SMEM, SMEM, VMEM, VMEM, VMEM, VMEM],
        out_specs=VMEM,
        name="attend",
    )(
        first,
        lengths,
        block_table[0],
        query_all,
        key_pool.reshape(SLOTS * BLOCK, KVH * DH),
        value_pool.reshape(SLOTS * BLOCK, KVH * DH),
    )
    collected = lax.all_to_all(partial, "blk", split_axis=0, concat_axis=0, tiled=True)
    return pl.pallas_call(
        combine_kernel,
        out_shape=jax.ShapeDtypeStruct((TOK, HEADS * DH), bf16),
        in_specs=[VMEM],
        out_specs=VMEM,
        name="combine",
    )(collected)


def solution(mesh):
    placed = (
        P(None, ("blk", "grp")),
        P("grp", "blk", None, None),
        P("grp", "blk", None, None),
        P("grp", None),
        P("grp", None, None),
    )
    return jax.shard_map(
        body, mesh=mesh, in_specs=placed, out_specs=P("grp", "blk"), check_vma=False
    )
```

```python
import math

import jax
import jax.numpy as jnp
from jax import lax
from jax.experimental import pallas as pl
from jax.experimental.pallas import tpu as pltpu
from jax.sharding import PartitionSpec as P

HQ = 64
KVH = 8
DH = 128
STEPS = 3
SEQS = 4
TOK = SEQS * STEPS
HEADS = 2
ROWS = HEADS * TOK
SLICES = 4
SLOTS = 8
BLOCK = 128
LANES = 128
SCALE = math.log2(math.e) / math.sqrt(DH)
LN2 = math.log(2.0)
EMPTY = -1e30

VMEM = pl.BlockSpec(memory_space=pltpu.VMEM)
HBM = pl.BlockSpec(memory_space=pltpu.HBM)
SMEM = pl.BlockSpec(memory_space=pltpu.SMEM)


PARAMS = pltpu.CompilerParams(vmem_limit_bytes=16 * 1024 * 1024)


def in_hbm(array):
    return pltpu.with_memory_space_constraint(array, pltpu.HBM)


def iota(shape, dim):
    return lax.broadcasted_iota(jnp.int32, shape, dim)


def pack_kernel(first_ref, len_hbm, table_hbm, q_hbm, out_ref, bias_ref, len_ref, table_ref, q_ref, sems):
    copies = [
        pltpu.make_async_copy(q_hbm, q_ref, sems.at[0]),
        pltpu.make_async_copy(table_hbm, table_ref, sems.at[1]),
        pltpu.make_async_copy(len_hbm, len_ref, sems.at[2]),
    ]
    for c in copies:
        c.start()
    copies[0].wait()
    groups, feats, _ = out_ref.shape
    q = q_ref[...].astype(jnp.float32)
    keep = iota((feats, LANES), 1) < TOK
    wide = jnp.concatenate([q, jnp.zeros((feats, 2 * LANES - q.shape[1]), jnp.float32)], axis=1)
    for g in range(groups):
        at = g * TOK
        shifted = wide if at == 0 else pltpu.roll(wide, 2 * LANES - at, 1)
        out_ref[g] = jnp.where(keep, shifted[:, :LANES], 0.0).astype(out_ref.dtype)
    copies[1].wait()
    copies[2].wait()
    lane4 = iota((SEQS, LANES), 1)
    sub4 = iota((SEQS, LANES), 0)
    lens = jnp.zeros((SEQS, LANES), jnp.int32)
    for q in range(SEQS):
        lens = jnp.where(sub4 == q, len_ref[0, q], lens)
    local = jnp.where(lane4 < lens, table_ref[...] - first_ref[0], -1)
    row = iota((ROWS, LANES), 0)
    seq = jnp.where(row >= TOK, row - TOK, row) // STEPS
    for s in range(SLOTS):
        hit = jnp.max((local == s).astype(jnp.float32), axis=1, keepdims=True)
        off = jnp.broadcast_to(jnp.where(hit > 0.0, 0.0, EMPTY), (SEQS, LANES))
        b = jnp.broadcast_to(off[0:1], (ROWS, LANES))
        for q in range(1, SEQS):
            b = jnp.where(seq == q, off[q : q + 1], b)
        bias_ref[:, s * BLOCK : (s + 1) * BLOCK] = b


def spread_kernel(a_ref, out_ref):
    row = iota((ROWS, LANES), 0)
    tok = jnp.where(row >= TOK, row - TOK, row)
    pick = (tok == iota((ROWS, LANES), 1)).astype(jnp.bfloat16)
    nt = (((1,), (1,)), ((), ()))
    first = lax.dot_general(pick, a_ref[:LANES, :], nt, preferred_element_type=jnp.float32)
    second = lax.dot_general(pick, a_ref[LANES:, :], nt, preferred_element_type=jnp.float32)
    rows = jnp.where(row < TOK, first, second).astype(out_ref.dtype)
    for b in range(out_ref.shape[0]):
        out_ref[b] = rows


def attend_kernel(bias_ref, q_ref, k_hbm, v_hbm, out_ref, k_ref, v_ref, sems):
    def load(k):
        cols = pl.ds(k * DH, DH)
        return (
            pltpu.make_async_copy(k_hbm.at[:, cols], k_ref.at[:, cols], sems.at[0, k]),
            pltpu.make_async_copy(v_hbm.at[:, cols], v_ref.at[:, cols], sems.at[1, k]),
        )

    loads = [load(k) for k in range(KVH)]
    for pair in loads:
        for c in pair:
            c.start()
    bias = jnp.concatenate([bias_ref[...]] * SLICES, axis=0)

    rows = SLICES * ROWS
    lane = iota((rows, LANES), 1)
    lse = jnp.zeros((rows, LANES), jnp.float32)
    nt = (((1,), (1,)), ((), ()))
    nn = (((1,), (0,)), ((), ()))
    for k in range(KVH):
        cols = slice(k * DH, (k + 1) * DH)
        loads[k][0].wait()
        qk = q_ref[k * SLICES : (k + 1) * SLICES].reshape(rows, DH)
        s = lax.dot_general(qk, k_ref[:, cols], nt, preferred_element_type=jnp.float32) + bias
        top = jnp.max(s, axis=1, keepdims=True)
        p = jnp.exp2((s - top) * SCALE).astype(jnp.bfloat16)
        total = jnp.sum(p.astype(jnp.float32), axis=1, keepdims=True)
        loads[k][1].wait()
        o = lax.dot_general(p, v_ref[:, cols], nn, preferred_element_type=jnp.float32)
        o = (o / total).astype(out_ref.dtype)
        lse = jnp.where(lane == k, top * SCALE + jnp.log2(total), lse)
        out_ref[k * SLICES : (k + 1) * SLICES, :ROWS, :] = o.reshape(SLICES, ROWS, DH)
    square = jnp.concatenate([lse, jnp.zeros((LANES - rows, LANES), jnp.float32)], axis=0)
    flat = jnp.transpose(square)[:KVH]
    lane8 = iota((KVH, LANES), 1)
    for j in range(SLICES):
        mine = flat if j == 0 else pltpu.roll(flat, LANES - j * ROWS, 1)
        mine = jnp.where(lane8 < ROWS, mine, 0.0)
        high = mine.astype(jnp.bfloat16).astype(jnp.float32)
        rest = mine - high
        mid = rest.astype(jnp.bfloat16).astype(jnp.float32)
        low = rest - mid
        line = high + pltpu.roll(mid, 32, 1) + pltpu.roll(low, 64, 1)
        for k in range(KVH):
            tile = jnp.broadcast_to(line[k : k + 1], (8, LANES))
            out_ref[k * SLICES + j, ROWS:, :] = tile.astype(out_ref.dtype)


def combine_kernel(a_ref, out_ref):
    devices = a_ref.shape[0]
    sub8 = iota((8, LANES), 0)
    parts = []
    for t in range(devices // 8):
        acc = a_ref[8 * t, ROWS:, :].astype(jnp.float32)
        for j in range(1, 8):
            acc = jnp.where(sub8 == j, a_ref[8 * t + j, ROWS:, :].astype(jnp.float32), acc)
        parts.append(acc)
    stat = jnp.concatenate(parts, axis=0)
    lse = stat + pltpu.roll(stat, LANES - 32, 1) + pltpu.roll(stat, LANES - 64, 1)
    top = jnp.max(lse, axis=0, keepdims=True)
    w = jnp.exp2(lse - top)
    w = w / jnp.sum(w, axis=0, keepdims=True)
    square = jnp.concatenate([w, jnp.zeros((LANES - devices, LANES), jnp.float32)], axis=0)
    wt = jnp.transpose(square)[:ROWS]
    acc = jnp.zeros((ROWS, LANES), jnp.float32)
    for b in range(devices):
        acc = acc + wt[:, b : b + 1] * a_ref[b, :ROWS, :].astype(jnp.float32)
    out_ref[...] = jnp.concatenate([acc[:TOK], acc[TOK:]], axis=1).astype(out_ref.dtype)


def body(queries, key_pool, value_pool, lengths, block_table):
    bf16 = jnp.bfloat16
    groups = lax.axis_size("grp")
    devices = lax.axis_size("blk")
    feats = queries.shape[1]
    first = (lax.axis_index("blk") * SLOTS).astype(jnp.int32).reshape(1)
    packed, bias = pl.pallas_call(
        pack_kernel,
        out_shape=(
            jax.ShapeDtypeStruct((groups, feats, LANES), bf16),
            jax.ShapeDtypeStruct((ROWS, SLOTS * BLOCK), jnp.float32),
        ),
        in_specs=[SMEM, HBM, HBM, HBM],
        out_specs=(VMEM, VMEM),
        scratch_shapes=[
            pltpu.SMEM(lengths.shape, jnp.int32),
            pltpu.VMEM(block_table.shape[1:], jnp.int32),
            pltpu.VMEM((feats, queries.shape[0]), bf16),
            pltpu.SemaphoreType.DMA((3,)),
        ],
        compiler_params=PARAMS,
        name="pack",
    )(first, in_hbm(lengths), in_hbm(block_table[0]), in_hbm(queries.T))
    arrived = lax.all_to_all(packed, "grp", split_axis=0, concat_axis=0, tiled=True)
    spread = pl.pallas_call(
        spread_kernel,
        out_shape=jax.ShapeDtypeStruct((devices, ROWS, LANES), bf16),
        in_specs=[VMEM],
        out_specs=VMEM,
        compiler_params=PARAMS,
        name="spread",
    )(arrived.reshape(groups * feats, LANES))
    query_all = lax.all_to_all(spread, "blk", split_axis=0, concat_axis=0, tiled=True)
    pool = (SLOTS * BLOCK, KVH * DH)
    partial = pl.pallas_call(
        attend_kernel,
        out_shape=jax.ShapeDtypeStruct((devices, ROWS + 8, LANES), bf16),
        in_specs=[VMEM, VMEM, HBM, HBM],
        out_specs=VMEM,
        scratch_shapes=[
            pltpu.VMEM(pool, bf16),
            pltpu.VMEM(pool, bf16),
            pltpu.SemaphoreType.DMA((2, KVH)),
        ],
        compiler_params=PARAMS,
        name="attend",
    )(bias, query_all, in_hbm(key_pool.reshape(pool)), in_hbm(value_pool.reshape(pool)))
    collected = lax.all_to_all(partial, "blk", split_axis=0, concat_axis=0, tiled=True)
    return pl.pallas_call(
        combine_kernel,
        out_shape=jax.ShapeDtypeStruct((TOK, HEADS * DH), bf16),
        in_specs=[VMEM],
        out_specs=VMEM,
        compiler_params=PARAMS,
        name="combine",
    )(collected)


def solution(mesh):
    placed = (
        P(None, ("blk", "grp")),
        P("grp", "blk", None, None),
        P("grp", "blk", None, None),
        P("grp", None),
        P("grp", None, None),
    )
    return jax.shard_map(
        body, mesh=mesh, in_specs=placed, out_specs=P("grp", "blk"), check_vma=False
    )
```

```python
import math

import jax
import jax.numpy as jnp
from jax import lax
from jax.experimental import pallas as pl
from jax.experimental.pallas import tpu as pltpu
from jax.sharding import PartitionSpec as P

HQ = 64
KVH = 8
DH = 128
STEPS = 3
SEQS = 4
TOK = SEQS * STEPS
HEADS = 2
ROWS = HEADS * TOK
SLICES = 4
SLOTS = 8
BLOCK = 128
FETCHES = 8
EARLY = 4
LANES = 128
SCALE = math.log2(math.e) / math.sqrt(DH)
LN2 = math.log(2.0)
EMPTY = -1e30

VMEM = pl.BlockSpec(memory_space=pltpu.VMEM)
HBM = pl.BlockSpec(memory_space=pltpu.HBM)
SMEM = pl.BlockSpec(memory_space=pltpu.SMEM)


PARAMS = pltpu.CompilerParams(vmem_limit_bytes=16 * 1024 * 1024)


def in_hbm(array):
    return pltpu.with_memory_space_constraint(array, pltpu.HBM)


def iota(shape, dim):
    return lax.broadcasted_iota(jnp.int32, shape, dim)


def pack_kernel(first_ref, len_hbm, table_hbm, q_hbm, out_ref, bias_ref, len_ref, table_ref, q_ref, sems):
    copies = [
        pltpu.make_async_copy(q_hbm, q_ref, sems.at[0]),
        pltpu.make_async_copy(table_hbm, table_ref, sems.at[1]),
        pltpu.make_async_copy(len_hbm, len_ref, sems.at[2]),
    ]
    for c in copies:
        c.start()
    copies[0].wait()
    groups, feats, _ = out_ref.shape
    q = q_ref[...].astype(jnp.float32)
    keep = iota((feats, LANES), 1) < TOK
    wide = jnp.concatenate([q, jnp.zeros((feats, 2 * LANES - q.shape[1]), jnp.float32)], axis=1)
    for g in range(groups):
        at = g * TOK
        shifted = wide if at == 0 else pltpu.roll(wide, 2 * LANES - at, 1)
        out_ref[g] = jnp.where(keep, shifted[:, :LANES], 0.0).astype(out_ref.dtype)
    copies[1].wait()
    copies[2].wait()
    lane4 = iota((SEQS, LANES), 1)
    sub4 = iota((SEQS, LANES), 0)
    lens = jnp.zeros((SEQS, LANES), jnp.int32)
    for q in range(SEQS):
        lens = jnp.where(sub4 == q, len_ref[0, q], lens)
    local = jnp.where(lane4 < lens, table_ref[...] - first_ref[0], -1)
    row = iota((ROWS, LANES), 0)
    seq = jnp.where(row >= TOK, row - TOK, row) // STEPS
    for s in range(SLOTS):
        hit = jnp.max((local == s).astype(jnp.float32), axis=1, keepdims=True)
        off = jnp.broadcast_to(jnp.where(hit > 0.0, 0.0, EMPTY), (SEQS, LANES))
        b = jnp.broadcast_to(off[0:1], (ROWS, LANES))
        for q in range(1, SEQS):
            b = jnp.where(seq == q, off[q : q + 1], b)
        bias_ref[:, s * BLOCK : (s + 1) * BLOCK] = b


def spread_kernel(a_ref, out_ref):
    row = iota((ROWS, LANES), 0)
    tok = jnp.where(row >= TOK, row - TOK, row)
    pick = (tok == iota((ROWS, LANES), 1)).astype(jnp.bfloat16)
    nt = (((1,), (1,)), ((), ()))
    first = lax.dot_general(pick, a_ref[:LANES, :], nt, preferred_element_type=jnp.float32)
    second = lax.dot_general(pick, a_ref[LANES:, :], nt, preferred_element_type=jnp.float32)
    rows = jnp.where(row < TOK, first, second).astype(out_ref.dtype)
    for b in range(out_ref.shape[0]):
        out_ref[b] = rows


def fetch_kernel(k_hbm, v_hbm, k_ref, v_ref, sems):
    rows = k_ref.shape[0] // FETCHES
    copies = []
    for i in range(FETCHES):
        at = pl.ds(i * rows, rows)
        copies.append(pltpu.make_async_copy(k_hbm.at[at], k_ref.at[at], sems.at[0, i]))
        copies.append(
            pltpu.make_async_copy(v_hbm.at[at, pl.ds(0, EARLY * DH)], v_ref.at[at], sems.at[1, i])
        )
    for c in copies:
        c.start()
    for c in copies:
        c.wait()


def attend_kernel(bias_ref, q_ref, k_ref, v_ref, v_hbm, out_ref, late_ref, sems):
    late = []
    for k in range(EARLY, KVH):
        to = pl.ds((k - EARLY) * DH, DH)
        late.append(
            pltpu.make_async_copy(
                v_hbm.at[:, pl.ds(k * DH, DH)], late_ref.at[:, to], sems.at[k - EARLY]
            )
        )
        late[-1].start()
    bias = jnp.concatenate([bias_ref[...]] * SLICES, axis=0)

    rows = SLICES * ROWS
    lane = iota((rows, LANES), 1)
    lse = jnp.zeros((rows, LANES), jnp.float32)
    nt = (((1,), (1,)), ((), ()))
    nn = (((1,), (0,)), ((), ()))
    for k in range(KVH):
        cols = slice(k * DH, (k + 1) * DH)
        qk = q_ref[k * SLICES : (k + 1) * SLICES].reshape(rows, DH)
        s = lax.dot_general(qk, k_ref[:, cols], nt, preferred_element_type=jnp.float32) + bias
        top = jnp.max(s, axis=1, keepdims=True)
        p = jnp.exp2((s - top) * SCALE).astype(jnp.bfloat16)
        total = jnp.sum(p.astype(jnp.float32), axis=1, keepdims=True)
        if k < EARLY:
            v = v_ref[:, cols]
        else:
            late[k - EARLY].wait()
            v = late_ref[:, (k - EARLY) * DH : (k - EARLY + 1) * DH]
        o = lax.dot_general(p, v, nn, preferred_element_type=jnp.float32)
        o = (o / total).astype(out_ref.dtype)
        lse = jnp.where(lane == k, top * SCALE + jnp.log2(total), lse)
        out_ref[k * SLICES : (k + 1) * SLICES, :ROWS, :] = o.reshape(SLICES, ROWS, DH)
    square = jnp.concatenate([lse, jnp.zeros((LANES - rows, LANES), jnp.float32)], axis=0)
    flat = jnp.transpose(square)[:KVH]
    lane8 = iota((KVH, LANES), 1)
    for j in range(SLICES):
        mine = flat if j == 0 else pltpu.roll(flat, LANES - j * ROWS, 1)
        mine = jnp.where(lane8 < ROWS, mine, 0.0)
        high = mine.astype(jnp.bfloat16).astype(jnp.float32)
        rest = mine - high
        mid = rest.astype(jnp.bfloat16).astype(jnp.float32)
        low = rest - mid
        line = high + pltpu.roll(mid, 32, 1) + pltpu.roll(low, 64, 1)
        for k in range(KVH):
            tile = jnp.broadcast_to(line[k : k + 1], (8, LANES))
            out_ref[k * SLICES + j, ROWS:, :] = tile.astype(out_ref.dtype)


def combine_kernel(a_ref, out_ref):
    devices = a_ref.shape[0]
    sub8 = iota((8, LANES), 0)
    parts = []
    for t in range(devices // 8):
        acc = a_ref[8 * t, ROWS:, :].astype(jnp.float32)
        for j in range(1, 8):
            acc = jnp.where(sub8 == j, a_ref[8 * t + j, ROWS:, :].astype(jnp.float32), acc)
        parts.append(acc)
    stat = jnp.concatenate(parts, axis=0)
    lse = stat + pltpu.roll(stat, LANES - 32, 1) + pltpu.roll(stat, LANES - 64, 1)
    top = jnp.max(lse, axis=0, keepdims=True)
    w = jnp.exp2(lse - top)
    w = w / jnp.sum(w, axis=0, keepdims=True)
    square = jnp.concatenate([w, jnp.zeros((LANES - devices, LANES), jnp.float32)], axis=0)
    wt = jnp.transpose(square)[:ROWS]
    acc = jnp.zeros((ROWS, LANES), jnp.float32)
    for b in range(devices):
        acc = acc + wt[:, b : b + 1] * a_ref[b, :ROWS, :].astype(jnp.float32)
    out_ref[...] = jnp.concatenate([acc[:TOK], acc[TOK:]], axis=1).astype(out_ref.dtype)


def body(queries, key_pool, value_pool, lengths, block_table):
    bf16 = jnp.bfloat16
    groups = lax.axis_size("grp")
    devices = lax.axis_size("blk")
    feats = queries.shape[1]
    first = (lax.axis_index("blk") * SLOTS).astype(jnp.int32).reshape(1)
    packed, bias = pl.pallas_call(
        pack_kernel,
        out_shape=(
            jax.ShapeDtypeStruct((groups, feats, LANES), bf16),
            jax.ShapeDtypeStruct((ROWS, SLOTS * BLOCK), jnp.float32),
        ),
        in_specs=[SMEM, HBM, HBM, HBM],
        out_specs=(VMEM, VMEM),
        scratch_shapes=[
            pltpu.SMEM(lengths.shape, jnp.int32),
            pltpu.VMEM(block_table.shape[1:], jnp.int32),
            pltpu.VMEM((feats, queries.shape[0]), bf16),
            pltpu.SemaphoreType.DMA((3,)),
        ],
        compiler_params=PARAMS,
        name="pack",
    )(first, in_hbm(lengths), in_hbm(block_table[0]), in_hbm(queries.T))
    arrived = lax.all_to_all(packed, "grp", split_axis=0, concat_axis=0, tiled=True)
    spread = pl.pallas_call(
        spread_kernel,
        out_shape=jax.ShapeDtypeStruct((devices, ROWS, LANES), bf16),
        in_specs=[VMEM],
        out_specs=VMEM,
        compiler_params=PARAMS,
        name="spread",
    )(arrived.reshape(groups * feats, LANES))
    pool = (SLOTS * BLOCK, KVH * DH)
    k_hbm = in_hbm(key_pool.reshape(pool))
    v_hbm = in_hbm(value_pool.reshape(pool))
    keys, values = pl.pallas_call(
        fetch_kernel,
        out_shape=(pltpu.VMEM(pool, bf16), pltpu.VMEM((pool[0], EARLY * DH), bf16)),
        in_specs=[HBM, HBM],
        out_specs=(VMEM, VMEM),
        scratch_shapes=[pltpu.SemaphoreType.DMA((2, FETCHES))],
        compiler_params=PARAMS,
        cost_estimate=pl.CostEstimate(flops=10**9, bytes_accessed=8 * 2**20, transcendentals=0),
        name="fetch",
    )(k_hbm, v_hbm)
    query_all = lax.all_to_all(spread, "blk", split_axis=0, concat_axis=0, tiled=True)
    partial = pl.pallas_call(
        attend_kernel,
        out_shape=jax.ShapeDtypeStruct((devices, ROWS + 8, LANES), bf16),
        in_specs=[VMEM, VMEM, VMEM, VMEM, HBM],
        out_specs=VMEM,
        scratch_shapes=[
            pltpu.VMEM((SLOTS * BLOCK, (KVH - EARLY) * DH), bf16),
            pltpu.SemaphoreType.DMA((KVH - EARLY,)),
        ],
        compiler_params=PARAMS,
        name="attend",
    )(bias, query_all, keys, values, v_hbm)
    collected = lax.all_to_all(partial, "blk", split_axis=0, concat_axis=0, tiled=True)
    return pl.pallas_call(
        combine_kernel,
        out_shape=jax.ShapeDtypeStruct((TOK, HEADS * DH), bf16),
        in_specs=[VMEM],
        out_specs=VMEM,
        compiler_params=PARAMS,
        name="combine",
    )(collected)


def solution(mesh):
    placed = (
        P(None, ("blk", "grp")),
        P("grp", "blk", None, None),
        P("grp", "blk", None, None),
        P("grp", None),
        P("grp", None, None),
    )
    return jax.shard_map(
        body, mesh=mesh, in_specs=placed, out_specs=P("grp", "blk"), check_vma=False
    )
```

```python
import math

import jax
import jax.numpy as jnp
from jax import lax
from jax.experimental import pallas as pl
from jax.experimental.pallas import tpu as pltpu
from jax.sharding import PartitionSpec as P

HQ = 64
KVH = 8
DH = 128
STEPS = 3
SEQS = 4
TOK = SEQS * STEPS
HEADS = 2
ROWS = HEADS * TOK
PART = HEADS * STEPS
SLICES = 4
SLOTS = 8
GAP = 32
LANES_A_SLOT = 16
BLOCK = 128
FETCHES = 8
EARLY = 4
LANES = 128
SCALE = math.log2(math.e) / math.sqrt(DH)
LN2 = math.log(2.0)
EMPTY = -1e30

VMEM = pl.BlockSpec(memory_space=pltpu.VMEM)
HBM = pl.BlockSpec(memory_space=pltpu.HBM)
SMEM = pl.BlockSpec(memory_space=pltpu.SMEM)


PARAMS = pltpu.CompilerParams(vmem_limit_bytes=16 * 1024 * 1024)


def in_hbm(array):
    return pltpu.with_memory_space_constraint(array, pltpu.HBM)


def iota(shape, dim):
    return lax.broadcasted_iota(jnp.int32, shape, dim)


def pack_kernel(q_ref, out_ref):
    groups, feats, _ = out_ref.shape
    q = q_ref[...].astype(jnp.float32)
    keep = iota((feats, LANES), 1) < TOK
    wide = jnp.concatenate([q, jnp.zeros((feats, 2 * LANES - q.shape[1]), jnp.float32)], axis=1)
    for g in range(groups):
        at = g * TOK
        shifted = wide if at == 0 else pltpu.roll(wide, 2 * LANES - at, 1)
        out_ref[g] = jnp.where(keep, shifted[:, :LANES], 0.0).astype(out_ref.dtype)


def spread_kernel(a_ref, out_ref):
    row = iota((ROWS, LANES), 0)
    tok = jnp.where(row >= TOK, row - TOK, row)
    pick = (tok == iota((ROWS, LANES), 1)).astype(jnp.bfloat16)
    nt = (((1,), (1,)), ((), ()))
    first = lax.dot_general(pick, a_ref[:LANES, :], nt, preferred_element_type=jnp.float32)
    second = lax.dot_general(pick, a_ref[LANES:, :], nt, preferred_element_type=jnp.float32)
    rows = jnp.where(row < TOK, first, second).astype(out_ref.dtype)
    for b in range(out_ref.shape[0]):
        out_ref[b] = rows


def place(q, r):
    slice_, rest = r // PART, r % PART
    return slice_ * ROWS + (rest // STEPS) * TOK + q * STEPS + rest % STEPS


def fetch_kernel(
    first_ref, len_hbm, table_hbm, k_hbm, v_hbm,
    k_ref, v_ref, gather_ref, scatter_ref, own_ref, owner_ref,
    len_ref, table_ref, sems, small,
):
    rows = k_ref.shape[0] // FETCHES
    copies = []
    for i in range(FETCHES):
        at = pl.ds(i * rows, rows)
        copies.append(pltpu.make_async_copy(k_hbm.at[at], k_ref.at[at], sems.at[0, i]))
        copies.append(
            pltpu.make_async_copy(v_hbm.at[at, pl.ds(0, EARLY * DH)], v_ref.at[at], sems.at[1, i])
        )
    facts = [
        pltpu.make_async_copy(table_hbm, table_ref, small.at[0]),
        pltpu.make_async_copy(len_hbm, len_ref, small.at[1]),
    ]
    for c in facts + copies:
        c.start()
    for c in facts:
        c.wait()
    lane4 = iota((SEQS, LANES), 1)
    sub4 = iota((SEQS, LANES), 0)
    lens = jnp.zeros((SEQS, LANES), jnp.int32)
    for q in range(SEQS):
        lens = jnp.where(sub4 == q, len_ref[0, q], lens)
    local = jnp.where(lane4 < lens, table_ref[...] - first_ref[0], -1)
    r = iota((GAP, LANES), 0)
    c = iota((GAP, LANES), 1)
    lane8 = iota((8, LANES), 1) // LANES_A_SLOT
    owner = jnp.full((8, LANES), -1, jnp.int32)
    for s in range(SLOTS):
        hit = jnp.max((local == s).astype(jnp.float32), axis=1, keepdims=True)
        own_ref[s * SEQS : (s + 1) * SEQS, :] = jnp.broadcast_to(hit, (SEQS, LANES))
        q = jnp.max(jnp.where(hit > 0.0, sub4[:, :1], -1).astype(jnp.float32), axis=0, keepdims=True)
        q = jnp.broadcast_to(q.astype(jnp.int32), (8, LANES))
        owner = jnp.where(lane8 == s, q, owner)
        q = jnp.broadcast_to(q[:1], (GAP, LANES))
        pick = (c == place(q, r)) & (r < SLICES * PART) & (q >= 0)
        gather_ref[s * GAP : (s + 1) * GAP, :] = pick.astype(jnp.float32).astype(jnp.bfloat16)
    owner_ref[...] = owner
    n = SEQS * SLICES * PART
    to = iota((n, LANES), 0)
    row = iota((n, LANES), 1)
    pick = (to == place(row // (SLICES * PART), row % (SLICES * PART))) & (row < n)
    scatter_ref[...] = pick.astype(jnp.float32).astype(jnp.bfloat16)
    for c in copies:
        c.wait()


def attend_kernel(
    gather_ref, scatter_ref, own_ref, owner_ref, q_ref, k_ref, v_ref, v_hbm,
    out_ref, late_ref, s_ref, sems,
):
    late = []
    for k in range(EARLY, KVH):
        to = pl.ds((k - EARLY) * DH, DH)
        late.append(
            pltpu.make_async_copy(
                v_hbm.at[:, pl.ds(k * DH, DH)], late_ref.at[:, to], sems.at[k - EARLY]
            )
        )
        late[-1].start()
    one = SLICES * PART
    rows = SEQS * one
    nt = (((1,), (1,)), ((), ()))
    nn = (((1,), (0,)), ((), ()))
    gather = gather_ref[:, :rows]
    scatter = scatter_ref[:, :rows]
    lane = iota((one, LANES), 1)

    top = jnp.full((one, LANES), EMPTY, jnp.float32)
    for k in range(KVH):
        cols = slice(k * DH, (k + 1) * DH)
        qk = q_ref[k * SLICES : (k + 1) * SLICES].reshape(rows, DH)
        qs = lax.dot_general(gather, qk, nn, preferred_element_type=jnp.float32)
        qs = qs.astype(jnp.bfloat16)
        for s in range(SLOTS):
            scores = lax.dot_general(
                qs[s * GAP : (s + 1) * GAP],
                k_ref[s * BLOCK : (s + 1) * BLOCK, cols],
                nt,
                preferred_element_type=jnp.float32,
            )[:one]
            s_ref[k * SLOTS + s] = scores
            most = jnp.max(scores, axis=1, keepdims=True)
            top = jnp.where(lane == s * LANES_A_SLOT + k, most, top)

    owner = jnp.concatenate([owner_ref[...]] * (one // 8), axis=0)
    slot_top = top
    seq_top = []
    for q in range(SEQS):
        t = jnp.where(owner == q, top, EMPTY)
        for shift in (16, 32, 64):
            t = jnp.maximum(t, pltpu.roll(t, shift, 1))
        seq_top.append(t)
        slot_top = jnp.where(owner == q, t, slot_top)

    wide = iota((rows, LANES), 1)
    totals = jnp.zeros((rows, LANES), jnp.float32)
    for k in range(KVH):
        cols = slice(k * DH, (k + 1) * DH)
        parts = [[] for _ in range(SEQS)]
        for s in range(SLOTS):
            at = s * LANES_A_SLOT + k
            p = jnp.exp2((s_ref[k * SLOTS + s] - slot_top[:, at : at + 1]) * SCALE)
            for q in range(SEQS):
                parts[q].append(p * own_ref[s * SEQS + q : s * SEQS + q + 1, :])
        sums = jnp.concatenate([sum(x[1:], x[0]) for x in parts], axis=0)
        total = jnp.sum(sums, axis=1, keepdims=True)
        p = jnp.concatenate(
            [
                jnp.concatenate([parts[q][s] for q in range(SEQS)], axis=0).astype(jnp.bfloat16)
                for s in range(SLOTS)
            ],
            axis=1,
        )
        if k < EARLY:
            v = v_ref[:, cols]
        else:
            late[k - EARLY].wait()
            v = late_ref[:, (k - EARLY) * DH : (k - EARLY + 1) * DH]
        o = lax.dot_general(p, v, nn, preferred_element_type=jnp.float32)
        o = jnp.where(total > 0.0, o / jnp.where(total > 0.0, total, 1.0), 0.0)
        o = lax.dot_general(
            scatter, o.astype(jnp.bfloat16), nn, preferred_element_type=jnp.float32
        ).astype(out_ref.dtype)
        out_ref[k * SLICES : (k + 1) * SLICES, :ROWS, :] = o.reshape(SLICES, ROWS, DH)
        totals = jnp.where(wide == k, total, totals)

    some = totals > 0.0
    lse = jnp.concatenate(seq_top, axis=0) * SCALE
    lse = jnp.where(some, lse + jnp.log2(jnp.where(some, totals, 1.0)), EMPTY)
    lse = jnp.where(wide < KVH, lse, 0.0)
    high = lse.astype(jnp.bfloat16).astype(jnp.float32)
    rest = lse - high
    mid = rest.astype(jnp.bfloat16).astype(jnp.float32)
    low = rest - mid
    pieces = high + pltpu.roll(mid, KVH, 1) + pltpu.roll(low, 2 * KVH, 1)
    pieces = lax.dot_general(
        scatter, pieces.astype(jnp.bfloat16), nn, preferred_element_type=jnp.float32
    )
    square = jnp.concatenate([pieces, jnp.zeros((LANES - rows, LANES), jnp.float32)], axis=0)
    flat = jnp.transpose(square)
    lane8 = iota((KVH, LANES), 1)
    for j in range(SLICES):
        line = jnp.zeros((KVH, LANES), jnp.float32)
        for i in range(3):
            shift = (32 * i - j * ROWS) % LANES
            part = flat[i * KVH : (i + 1) * KVH]
            part = part if shift == 0 else pltpu.roll(part, shift, 1)
            line = jnp.where((lane8 >= 32 * i) & (lane8 < 32 * i + ROWS), part, line)
        for k in range(KVH):
            tile = jnp.broadcast_to(line[k : k + 1], (8, LANES))
            out_ref[k * SLICES + j, ROWS:, :] = tile.astype(out_ref.dtype)


def combine_kernel(a_ref, out_ref):
    devices = a_ref.shape[0]
    sub8 = iota((8, LANES), 0)
    parts = []
    for t in range(devices // 8):
        acc = a_ref[8 * t, ROWS:, :].astype(jnp.float32)
        for j in range(1, 8):
            acc = jnp.where(sub8 == j, a_ref[8 * t + j, ROWS:, :].astype(jnp.float32), acc)
        parts.append(acc)
    stat = jnp.concatenate(parts, axis=0)
    lse = stat + pltpu.roll(stat, LANES - 32, 1) + pltpu.roll(stat, LANES - 64, 1)
    top = jnp.max(lse, axis=0, keepdims=True)
    w = jnp.exp2(lse - top)
    w = w / jnp.sum(w, axis=0, keepdims=True)
    square = jnp.concatenate([w, jnp.zeros((LANES - devices, LANES), jnp.float32)], axis=0)
    wt = jnp.transpose(square)[:ROWS]
    acc = jnp.zeros((ROWS, LANES), jnp.float32)
    for b in range(devices):
        acc = acc + wt[:, b : b + 1] * a_ref[b, :ROWS, :].astype(jnp.float32)
    out_ref[...] = jnp.concatenate([acc[:TOK], acc[TOK:]], axis=1).astype(out_ref.dtype)


def body(queries, key_pool, value_pool, lengths, block_table):
    bf16 = jnp.bfloat16
    groups = lax.axis_size("grp")
    devices = lax.axis_size("blk")
    feats = queries.shape[1]
    first = (lax.axis_index("blk") * SLOTS).astype(jnp.int32).reshape(1)
    packed = pl.pallas_call(
        pack_kernel,
        out_shape=jax.ShapeDtypeStruct((groups, feats, LANES), bf16),
        in_specs=[VMEM],
        out_specs=VMEM,
        compiler_params=PARAMS,
        name="pack",
    )(queries.T)
    arrived = lax.all_to_all(packed, "grp", split_axis=0, concat_axis=0, tiled=True)
    spread = pl.pallas_call(
        spread_kernel,
        out_shape=jax.ShapeDtypeStruct((devices, ROWS, LANES), bf16),
        in_specs=[VMEM],
        out_specs=VMEM,
        compiler_params=PARAMS,
        name="spread",
    )(arrived.reshape(groups * feats, LANES))
    pool = (SLOTS * BLOCK, KVH * DH)
    k_hbm = in_hbm(key_pool.reshape(pool))
    v_hbm = in_hbm(value_pool.reshape(pool))
    lines = SEQS * SLICES * PART
    keys, values, gather, scatter, own, owner = pl.pallas_call(
        fetch_kernel,
        out_shape=(
            pltpu.VMEM(pool, bf16),
            pltpu.VMEM((pool[0], EARLY * DH), bf16),
            pltpu.VMEM((SLOTS * GAP, LANES), bf16),
            pltpu.VMEM((lines, LANES), bf16),
            pltpu.VMEM((SLOTS * SEQS, LANES), jnp.float32),
            pltpu.VMEM((8, LANES), jnp.int32),
        ),
        in_specs=[SMEM, HBM, HBM, HBM, HBM],
        out_specs=(VMEM,) * 6,
        scratch_shapes=[
            pltpu.SMEM(lengths.shape, jnp.int32),
            pltpu.VMEM(block_table.shape[1:], jnp.int32),
            pltpu.SemaphoreType.DMA((2, FETCHES)),
            pltpu.SemaphoreType.DMA((2,)),
        ],
        compiler_params=PARAMS,
        cost_estimate=pl.CostEstimate(flops=10**9, bytes_accessed=8 * 2**20, transcendentals=0),
        name="fetch",
    )(first, in_hbm(lengths), in_hbm(block_table[0]), k_hbm, v_hbm)
    query_all = lax.all_to_all(spread, "blk", split_axis=0, concat_axis=0, tiled=True)
    partial = pl.pallas_call(
        attend_kernel,
        out_shape=jax.ShapeDtypeStruct((devices, ROWS + 8, LANES), bf16),
        in_specs=[VMEM] * 7 + [HBM],
        out_specs=VMEM,
        scratch_shapes=[
            pltpu.VMEM((SLOTS * BLOCK, (KVH - EARLY) * DH), bf16),
            pltpu.VMEM((KVH * SLOTS, SLICES * PART, LANES), jnp.float32),
            pltpu.SemaphoreType.DMA((KVH - EARLY,)),
        ],
        compiler_params=PARAMS,
        name="attend",
    )(gather, scatter, own, owner, query_all, keys, values, v_hbm)
    collected = lax.all_to_all(partial, "blk", split_axis=0, concat_axis=0, tiled=True)
    return pl.pallas_call(
        combine_kernel,
        out_shape=jax.ShapeDtypeStruct((TOK, HEADS * DH), bf16),
        in_specs=[VMEM],
        out_specs=VMEM,
        compiler_params=PARAMS,
        name="combine",
    )(collected)


def solution(mesh):
    placed = (
        P(None, ("blk", "grp")),
        P("grp", "blk", None, None),
        P("grp", "blk", None, None),
        P("grp", None),
        P("grp", None, None),
    )
    return jax.shard_map(
        body, mesh=mesh, in_specs=placed, out_specs=P("grp", "blk"), check_vma=False
    )
```

```python
import math

import jax
import jax.numpy as jnp
from jax import lax
from jax.experimental import pallas as pl
from jax.experimental.pallas import tpu as pltpu
from jax.sharding import PartitionSpec as P

HQ = 64
KVH = 8
DH = 128
STEPS = 3
SEQS = 4
TOK = SEQS * STEPS
HEADS = 2
ROWS = HEADS * TOK
SLICES = 4
SLOTS = 8
WIDE = 256
CHUNK = 16
BLOCK = 128
FETCHES = 8
LATE = 6
EARLY = 4
LANES = 128
SCALE = math.log2(math.e) / math.sqrt(DH)
LN2 = math.log(2.0)
EMPTY = -1e30

VMEM = pl.BlockSpec(memory_space=pltpu.VMEM)
HBM = pl.BlockSpec(memory_space=pltpu.HBM)
SMEM = pl.BlockSpec(memory_space=pltpu.SMEM)


PARAMS = pltpu.CompilerParams(vmem_limit_bytes=16 * 1024 * 1024)


def in_hbm(array):
    return pltpu.with_memory_space_constraint(array, pltpu.HBM)


def iota(shape, dim):
    return lax.broadcasted_iota(jnp.int32, shape, dim)


def pack_kernel(q_ref, out_ref):
    groups, feats, _ = out_ref.shape
    q = q_ref[...].astype(jnp.float32)
    keep = iota((feats, LANES), 1) < TOK
    wide = jnp.concatenate([q, jnp.zeros((feats, 2 * LANES - q.shape[1]), jnp.float32)], axis=1)
    for g in range(groups):
        at = g * TOK
        shifted = wide if at == 0 else pltpu.roll(wide, 2 * LANES - at, 1)
        out_ref[g] = jnp.where(keep, shifted[:, :LANES], 0.0).astype(out_ref.dtype)


def spread_kernel(a_ref, out_ref):
    row = iota((ROWS, LANES), 0)
    tok = jnp.where(row >= TOK, row - TOK, row)
    pick = (tok == iota((ROWS, LANES), 1)).astype(jnp.bfloat16)
    nt = (((1,), (1,)), ((), ()))
    first = lax.dot_general(pick, a_ref[:LANES, :], nt, preferred_element_type=jnp.float32)
    second = lax.dot_general(pick, a_ref[LANES:, :], nt, preferred_element_type=jnp.float32)
    rows = jnp.where(row < TOK, first, second).astype(out_ref.dtype)
    for b in range(out_ref.shape[0]):
        out_ref[b] = rows


def fetch_kernel(
    first_ref, len_hbm, table_hbm, k_hbm, v_hbm,
    k_ref, v_ref, bias_ref, len_ref, table_ref, sems, small,
):
    rows = k_ref.shape[0] // FETCHES
    copies = []
    for i in range(FETCHES):
        at = pl.ds(i * rows, rows)
        copies.append(pltpu.make_async_copy(k_hbm.at[at], k_ref.at[at], sems.at[0, i]))
        copies.append(
            pltpu.make_async_copy(v_hbm.at[at, pl.ds(0, EARLY * DH)], v_ref.at[at], sems.at[1, i])
        )
    facts = [
        pltpu.make_async_copy(table_hbm, table_ref, small.at[0]),
        pltpu.make_async_copy(len_hbm, len_ref, small.at[1]),
    ]
    for c in facts + copies:
        c.start()
    for c in facts:
        c.wait()
    lane4 = iota((SEQS, LANES), 1)
    sub4 = iota((SEQS, LANES), 0)
    lens = jnp.zeros((SEQS, LANES), jnp.int32)
    for q in range(SEQS):
        lens = jnp.where(sub4 == q, len_ref[0, q], lens)
    local = jnp.where(lane4 < lens, table_ref[...] - first_ref[0], -1)
    row = iota((ROWS, LANES), 0)
    seq = jnp.where(row >= TOK, row - TOK, row) // STEPS
    for s in range(SLOTS):
        hit = jnp.max((local == s).astype(jnp.float32), axis=1, keepdims=True)
        off = jnp.broadcast_to(jnp.where(hit > 0.0, 0.0, EMPTY), (SEQS, LANES))
        b = jnp.broadcast_to(off[0:1], (ROWS, LANES))
        for q in range(1, SEQS):
            b = jnp.where(seq == q, off[q : q + 1], b)
        bias_ref[:, s * BLOCK : (s + 1) * BLOCK] = b
    for c in copies:
        c.wait()


def attend_kernel(
    bias_ref, q_ref, k_ref, v_ref, v_hbm, out_ref, late_ref, s_ref, p_ref, top_ref, sum_ref, sems
):
    late = []
    for k in range(EARLY, KVH):
        to = pl.ds((k - EARLY) * DH, DH)
        late.append(
            pltpu.make_async_copy(
                v_hbm.at[:, pl.ds(k * DH, DH)], late_ref.at[:, to], sems.at[k - EARLY]
            )
        )
        late[-1].start()
    rows = SLICES * ROWS
    lane = iota((rows, LANES), 1)
    lse = jnp.zeros((rows, LANES), jnp.float32)
    nt = (((1,), (1,)), ((), ()))
    nn = (((1,), (0,)), ((), ()))

    def cols(k):
        return slice(k * DH, (k + 1) * DH)

    def scores(k):
        qk = q_ref[k * SLICES : (k + 1) * SLICES].reshape(rows, DH)
        most = None
        for j in range(0, SLOTS * BLOCK, WIDE):
            at = slice(j, j + WIDE)
            s = lax.dot_general(qk, k_ref[at, cols(k)], nt, preferred_element_type=jnp.float32)
            s = s + jnp.concatenate([bias_ref[:, at]] * SLICES, axis=0)
            s_ref[k % 2, :, at] = s
            for i in range(0, WIDE, LANES):
                part = s[:, i : i + LANES]
                most = part if most is None else jnp.maximum(most, part)
        top = jnp.max(most, axis=1, keepdims=True)
        top_ref[k] = jnp.broadcast_to(top, (rows, LANES))

    def weights(k):
        for r in range(0, rows, CHUNK):
            at = slice(r, r + CHUNK)
            top = top_ref[k, at]
            total = None
            for j in range(0, SLOTS * BLOCK, LANES):
                here = slice(j, j + LANES)
                p = jnp.exp2((s_ref[k % 2, at, here] - top) * SCALE)
                total = p if total is None else total + p
                p_ref[k % 2, at, here] = p.astype(jnp.bfloat16)
            sum_ref[k % 2, at] = total

    def values(k, lse):
        if k < EARLY:
            v = v_ref[:, cols(k)]
        else:
            v = late_ref[:, cols(k - EARLY)]
        o = lax.dot_general(p_ref[k % 2], v, nn, preferred_element_type=jnp.float32)
        total = jnp.sum(sum_ref[k % 2], axis=1, keepdims=True)
        o = (o * (1.0 / total)).astype(out_ref.dtype)
        out_ref[k * SLICES : (k + 1) * SLICES, :ROWS, :] = o.reshape(SLICES, ROWS, DH)
        return jnp.where(lane == k, top_ref[k] * SCALE + jnp.log2(total), lse)

    for step in range(KVH + 2):
        if step == LATE:
            for c in late:
                c.wait()
        if step < KVH:
            scores(step)
        if 0 <= step - 1 < KVH:
            weights(step - 1)
        if step >= 2:
            lse = values(step - 2, lse)
    square = jnp.concatenate([lse, jnp.zeros((LANES - rows, LANES), jnp.float32)], axis=0)
    flat = jnp.transpose(square)[:KVH]
    lane8 = iota((KVH, LANES), 1)
    for j in range(SLICES):
        mine = flat if j == 0 else pltpu.roll(flat, LANES - j * ROWS, 1)
        mine = jnp.where(lane8 < ROWS, mine, 0.0)
        high = mine.astype(jnp.bfloat16).astype(jnp.float32)
        rest = mine - high
        mid = rest.astype(jnp.bfloat16).astype(jnp.float32)
        low = rest - mid
        line = high + pltpu.roll(mid, 32, 1) + pltpu.roll(low, 64, 1)
        for k in range(KVH):
            tile = jnp.broadcast_to(line[k : k + 1], (8, LANES))
            out_ref[k * SLICES + j, ROWS:, :] = tile.astype(out_ref.dtype)


def combine_kernel(a_ref, out_ref):
    devices = a_ref.shape[0]
    sub8 = iota((8, LANES), 0)
    parts = []
    for t in range(devices // 8):
        acc = a_ref[8 * t, ROWS:, :].astype(jnp.float32)
        for j in range(1, 8):
            acc = jnp.where(sub8 == j, a_ref[8 * t + j, ROWS:, :].astype(jnp.float32), acc)
        parts.append(acc)
    stat = jnp.concatenate(parts, axis=0)
    lse = stat + pltpu.roll(stat, LANES - 32, 1) + pltpu.roll(stat, LANES - 64, 1)
    top = jnp.max(lse, axis=0, keepdims=True)
    w = jnp.exp2(lse - top)
    w = w / jnp.sum(w, axis=0, keepdims=True)
    square = jnp.concatenate([w, jnp.zeros((LANES - devices, LANES), jnp.float32)], axis=0)
    wt = jnp.transpose(square)[:ROWS]
    acc = jnp.zeros((ROWS, LANES), jnp.float32)
    for b in range(devices):
        acc = acc + wt[:, b : b + 1] * a_ref[b, :ROWS, :].astype(jnp.float32)
    out_ref[...] = jnp.concatenate([acc[:TOK], acc[TOK:]], axis=1).astype(out_ref.dtype)


def body(queries, key_pool, value_pool, lengths, block_table):
    bf16 = jnp.bfloat16
    groups = lax.axis_size("grp")
    devices = lax.axis_size("blk")
    feats = queries.shape[1]
    first = (lax.axis_index("blk") * SLOTS).astype(jnp.int32).reshape(1)
    packed = pl.pallas_call(
        pack_kernel,
        out_shape=jax.ShapeDtypeStruct((groups, feats, LANES), bf16),
        in_specs=[VMEM],
        out_specs=VMEM,
        compiler_params=PARAMS,
        name="pack",
    )(queries.T)
    arrived = lax.all_to_all(packed, "grp", split_axis=0, concat_axis=0, tiled=True)
    spread = pl.pallas_call(
        spread_kernel,
        out_shape=jax.ShapeDtypeStruct((devices, ROWS, LANES), bf16),
        in_specs=[VMEM],
        out_specs=VMEM,
        compiler_params=PARAMS,
        name="spread",
    )(arrived.reshape(groups * feats, LANES))
    pool = (SLOTS * BLOCK, KVH * DH)
    k_hbm = in_hbm(key_pool.reshape(pool))
    v_hbm = in_hbm(value_pool.reshape(pool))
    keys, values, bias = pl.pallas_call(
        fetch_kernel,
        out_shape=(
            pltpu.VMEM(pool, bf16),
            pltpu.VMEM((pool[0], EARLY * DH), bf16),
            pltpu.VMEM((ROWS, pool[0]), jnp.float32),
        ),
        in_specs=[SMEM, HBM, HBM, HBM, HBM],
        out_specs=(VMEM,) * 3,
        scratch_shapes=[
            pltpu.SMEM(lengths.shape, jnp.int32),
            pltpu.VMEM(block_table.shape[1:], jnp.int32),
            pltpu.SemaphoreType.DMA((2, FETCHES)),
            pltpu.SemaphoreType.DMA((2,)),
        ],
        compiler_params=PARAMS,
        cost_estimate=pl.CostEstimate(flops=10**9, bytes_accessed=8 * 2**20, transcendentals=0),
        name="fetch",
    )(first, in_hbm(lengths), in_hbm(block_table[0]), k_hbm, v_hbm)
    query_all = lax.all_to_all(spread, "blk", split_axis=0, concat_axis=0, tiled=True)
    rows = SLICES * ROWS
    partial = pl.pallas_call(
        attend_kernel,
        out_shape=jax.ShapeDtypeStruct((devices, ROWS + 8, LANES), bf16),
        in_specs=[VMEM] * 4 + [HBM],
        out_specs=VMEM,
        scratch_shapes=[
            pltpu.VMEM((pool[0], (KVH - EARLY) * DH), bf16),
            pltpu.VMEM((2, rows, pool[0]), jnp.float32),
            pltpu.VMEM((2, rows, pool[0]), bf16),
            pltpu.VMEM((KVH, rows, LANES), jnp.float32),
            pltpu.VMEM((2, rows, LANES), jnp.float32),
            pltpu.SemaphoreType.DMA((KVH - EARLY,)),
        ],
        compiler_params=PARAMS,
        name="attend",
    )(bias, query_all, keys, values, v_hbm)
    collected = lax.all_to_all(partial, "blk", split_axis=0, concat_axis=0, tiled=True)
    return pl.pallas_call(
        combine_kernel,
        out_shape=jax.ShapeDtypeStruct((TOK, HEADS * DH), bf16),
        in_specs=[VMEM],
        out_specs=VMEM,
        compiler_params=PARAMS,
        name="combine",
    )(collected)


def solution(mesh):
    placed = (
        P(None, ("blk", "grp")),
        P("grp", "blk", None, None),
        P("grp", "blk", None, None),
        P("grp", None),
        P("grp", None, None),
    )
    return jax.shard_map(
        body, mesh=mesh, in_specs=placed, out_specs=P("grp", "blk"), check_vma=False
    )
```

```python
import math

import jax
import jax.numpy as jnp
from jax import lax
from jax.experimental import pallas as pl
from jax.experimental.pallas import tpu as pltpu
from jax.sharding import PartitionSpec as P

HQ = 64
KVH = 8
DH = 128
STEPS = 3
SEQS = 4
TOK = SEQS * STEPS
HEADS = 2
ROWS = HEADS * TOK
SLICES = 4
SLOTS = 8
WIDE = 256
CHUNK = 16
BLOCK = 128
FETCHES = 8
LATE = 6
EARLY = 4
LANES = 128
HALF_FEATS = 8
HALF = 16
SCALE = math.log2(math.e) / math.sqrt(DH)
LN2 = math.log(2.0)
EMPTY = -1e30

VMEM = pl.BlockSpec(memory_space=pltpu.VMEM)
HBM = pl.BlockSpec(memory_space=pltpu.HBM)
SMEM = pl.BlockSpec(memory_space=pltpu.SMEM)


PARAMS = pltpu.CompilerParams(vmem_limit_bytes=16 * 1024 * 1024)


def in_hbm(array):
    return pltpu.with_memory_space_constraint(array, pltpu.HBM)


def iota(shape, dim):
    return lax.broadcasted_iota(jnp.int32, shape, dim)


def pack_kernel(q_ref, out_ref):
    groups, feats, _ = out_ref.shape
    q = q_ref[...].astype(jnp.float32)
    lane = iota((feats, LANES), 1)
    wide = jnp.concatenate([q, jnp.zeros((2 * feats, 2 * LANES - q.shape[1]), jnp.float32)], axis=1)

    def turned(part, shift):
        shift %= 2 * LANES
        return (part if shift == 0 else pltpu.roll(part, shift, 1))[:, :LANES]

    for g in range(groups):
        low = turned(wide[:feats], -g * TOK)
        high = turned(wide[feats:], HALF - g * TOK)
        both = jnp.where(lane < TOK, low, jnp.where((lane >= HALF) & (lane < HALF + TOK), high, 0.0))
        out_ref[g] = both.astype(out_ref.dtype)


def spread_kernel(a_ref, out_ref):
    feats = a_ref.shape[0]
    row = iota((ROWS, LANES), 0)
    tok = jnp.where(row >= TOK, row - TOK, row)
    lane = iota((ROWS, LANES), 1)
    nt = (((1,), (1,)), ((), ()))
    nn = (((1,), (0,)), ((), ()))
    halves = []
    for j in range(2):
        pick = (lane == tok + j * HALF).astype(jnp.bfloat16)
        halves.append(lax.dot_general(pick, a_ref[...], nt, preferred_element_type=jnp.float32))
    apart = jnp.concatenate(halves, axis=1).astype(jnp.bfloat16)
    at = iota((2 * feats, 2 * feats), 0)
    to = iota((2 * feats, 2 * feats), 1)
    second = at >= feats
    at = jnp.where(second, at - feats, at)
    order = to == (at // HALF_FEATS) * (2 * HALF_FEATS) + at % HALF_FEATS + jnp.where(second, HALF_FEATS, 0)
    whole = lax.dot_general(
        apart, order.astype(jnp.bfloat16), nn, preferred_element_type=jnp.float32
    )
    rows = jnp.where(row < TOK, whole[:, :LANES], whole[:, LANES:]).astype(out_ref.dtype)
    for b in range(out_ref.shape[0]):
        out_ref[b] = rows


def fetch_kernel(
    first_ref, len_hbm, table_hbm, k_hbm, v_hbm,
    k_ref, v_ref, bias_ref, len_ref, table_ref, sems, small,
):
    rows = k_ref.shape[0] // FETCHES
    copies = []
    for i in range(FETCHES):
        at = pl.ds(i * rows, rows)
        copies.append(pltpu.make_async_copy(k_hbm.at[at], k_ref.at[at], sems.at[0, i]))
        copies.append(
            pltpu.make_async_copy(v_hbm.at[at, pl.ds(0, EARLY * DH)], v_ref.at[at], sems.at[1, i])
        )
    facts = [
        pltpu.make_async_copy(table_hbm, table_ref, small.at[0]),
        pltpu.make_async_copy(len_hbm, len_ref, small.at[1]),
    ]
    for c in facts + copies:
        c.start()
    for c in facts:
        c.wait()
    lane4 = iota((SEQS, LANES), 1)
    sub4 = iota((SEQS, LANES), 0)
    lens = jnp.zeros((SEQS, LANES), jnp.int32)
    for q in range(SEQS):
        lens = jnp.where(sub4 == q, len_ref[0, q], lens)
    local = jnp.where(lane4 < lens, table_ref[...] - first_ref[0], -1)
    row = iota((ROWS, LANES), 0)
    seq = jnp.where(row >= TOK, row - TOK, row) // STEPS
    for s in range(SLOTS):
        hit = jnp.max((local == s).astype(jnp.float32), axis=1, keepdims=True)
        off = jnp.broadcast_to(jnp.where(hit > 0.0, 0.0, EMPTY), (SEQS, LANES))
        b = jnp.broadcast_to(off[0:1], (ROWS, LANES))
        for q in range(1, SEQS):
            b = jnp.where(seq == q, off[q : q + 1], b)
        bias_ref[:, s * BLOCK : (s + 1) * BLOCK] = b
    for c in copies:
        c.wait()


def attend_kernel(
    bias_ref, q_ref, k_ref, v_ref, v_hbm, out_ref, late_ref, s_ref, p_ref, top_ref, sum_ref, sems
):
    late = []
    for k in range(EARLY, KVH):
        to = pl.ds((k - EARLY) * DH, DH)
        late.append(
            pltpu.make_async_copy(
                v_hbm.at[:, pl.ds(k * DH, DH)], late_ref.at[:, to], sems.at[k - EARLY]
            )
        )
        late[-1].start()
    rows = SLICES * ROWS
    lane = iota((rows, LANES), 1)
    lse = jnp.zeros((rows, LANES), jnp.float32)
    nt = (((1,), (1,)), ((), ()))
    nn = (((1,), (0,)), ((), ()))

    def cols(k):
        return slice(k * DH, (k + 1) * DH)

    def scores(k):
        qk = q_ref[k * SLICES : (k + 1) * SLICES].reshape(rows, DH)
        most = None
        for j in range(0, SLOTS * BLOCK, WIDE):
            at = slice(j, j + WIDE)
            s = lax.dot_general(qk, k_ref[at, cols(k)], nt, preferred_element_type=jnp.float32)
            s = s + jnp.concatenate([bias_ref[:, at]] * SLICES, axis=0)
            s_ref[k % 2, :, at] = s
            for i in range(0, WIDE, LANES):
                part = s[:, i : i + LANES]
                most = part if most is None else jnp.maximum(most, part)
        top = jnp.max(most, axis=1, keepdims=True)
        top_ref[k] = jnp.broadcast_to(top, (rows, LANES))

    def weights(k, lse):
        for r in range(0, rows, CHUNK):
            at = slice(r, r + CHUNK)
            top = top_ref[k, at]
            total = None
            for j in range(0, SLOTS * BLOCK, LANES):
                here = slice(j, j + LANES)
                p = jnp.exp2((s_ref[k % 2, at, here] - top) * SCALE)
                total = p if total is None else total + p
                p_ref[k % 2, at, here] = p.astype(jnp.bfloat16)
            sum_ref[k % 2, at] = jnp.broadcast_to(
                jnp.sum(total, axis=1, keepdims=True), (CHUNK, LANES)
            )
        return jnp.where(lane == k, top_ref[k] * SCALE + jnp.log2(sum_ref[k % 2]), lse)

    def values(k):
        if k < EARLY:
            v = v_ref[:, cols(k)]
        else:
            v = late_ref[:, cols(k - EARLY)]
        o = lax.dot_general(p_ref[k % 2], v, nn, preferred_element_type=jnp.float32)
        o = (o * (1.0 / sum_ref[k % 2])).astype(out_ref.dtype)
        out_ref[k * SLICES : (k + 1) * SLICES, :ROWS, :] = o.reshape(SLICES, ROWS, DH)

    for step in range(KVH + 2):
        if step == LATE:
            for c in late:
                c.wait()
        if step < KVH:
            scores(step)
        if 0 <= step - 1 < KVH:
            lse = weights(step - 1, lse)
        if step >= 2:
            values(step - 2)
    square = jnp.concatenate([lse, jnp.zeros((LANES - rows, LANES), jnp.float32)], axis=0)
    flat = jnp.transpose(square)[:KVH]
    lane8 = iota((KVH, LANES), 1)
    for j in range(SLICES):
        mine = flat if j == 0 else pltpu.roll(flat, LANES - j * ROWS, 1)
        mine = jnp.where(lane8 < ROWS, mine, 0.0)
        high = mine.astype(jnp.bfloat16).astype(jnp.float32)
        rest = mine - high
        mid = rest.astype(jnp.bfloat16).astype(jnp.float32)
        low = rest - mid
        line = high + pltpu.roll(mid, 32, 1) + pltpu.roll(low, 64, 1)
        for k in range(KVH):
            tile = jnp.broadcast_to(line[k : k + 1], (8, LANES))
            out_ref[k * SLICES + j, ROWS:, :] = tile.astype(out_ref.dtype)


def combine_kernel(a_ref, out_ref):
    devices = a_ref.shape[0]
    sub8 = iota((8, LANES), 0)
    parts = []
    for t in range(devices // 8):
        acc = a_ref[8 * t, ROWS:, :].astype(jnp.float32)
        for j in range(1, 8):
            acc = jnp.where(sub8 == j, a_ref[8 * t + j, ROWS:, :].astype(jnp.float32), acc)
        parts.append(acc)
    stat = jnp.concatenate(parts, axis=0)
    lse = stat + pltpu.roll(stat, LANES - 32, 1) + pltpu.roll(stat, LANES - 64, 1)
    top = jnp.max(lse, axis=0, keepdims=True)
    w = jnp.exp2(lse - top)
    w = w / jnp.sum(w, axis=0, keepdims=True)
    square = jnp.concatenate([w, jnp.zeros((LANES - devices, LANES), jnp.float32)], axis=0)
    wt = jnp.transpose(square)[:ROWS]
    acc = jnp.zeros((ROWS, LANES), jnp.float32)
    for b in range(devices):
        acc = acc + wt[:, b : b + 1] * a_ref[b, :ROWS, :].astype(jnp.float32)
    out_ref[...] = jnp.concatenate([acc[:TOK], acc[TOK:]], axis=1).astype(out_ref.dtype)


def body(queries, key_pool, value_pool, lengths, block_table):
    bf16 = jnp.bfloat16
    groups = lax.axis_size("grp")
    devices = lax.axis_size("blk")
    first = (lax.axis_index("blk") * SLOTS).astype(jnp.int32).reshape(1)
    packed = pl.pallas_call(
        pack_kernel,
        out_shape=jax.ShapeDtypeStruct((groups, HALF_FEATS, LANES), bf16),
        in_specs=[VMEM],
        out_specs=VMEM,
        compiler_params=PARAMS,
        name="pack",
    )(queries.T)
    arrived = lax.all_to_all(packed, "grp", split_axis=0, concat_axis=0, tiled=True)
    spread = pl.pallas_call(
        spread_kernel,
        out_shape=jax.ShapeDtypeStruct((devices, ROWS, LANES), bf16),
        in_specs=[VMEM],
        out_specs=VMEM,
        compiler_params=PARAMS,
        name="spread",
    )(arrived.reshape(groups * HALF_FEATS, LANES))
    pool = (SLOTS * BLOCK, KVH * DH)
    k_hbm = in_hbm(key_pool.reshape(pool))
    v_hbm = in_hbm(value_pool.reshape(pool))
    keys, values, bias = pl.pallas_call(
        fetch_kernel,
        out_shape=(
            pltpu.VMEM(pool, bf16),
            pltpu.VMEM((pool[0], EARLY * DH), bf16),
            pltpu.VMEM((ROWS, pool[0]), jnp.float32),
        ),
        in_specs=[SMEM, HBM, HBM, HBM, HBM],
        out_specs=(VMEM,) * 3,
        scratch_shapes=[
            pltpu.SMEM(lengths.shape, jnp.int32),
            pltpu.VMEM(block_table.shape[1:], jnp.int32),
            pltpu.SemaphoreType.DMA((2, FETCHES)),
            pltpu.SemaphoreType.DMA((2,)),
        ],
        compiler_params=PARAMS,
        cost_estimate=pl.CostEstimate(flops=10**9, bytes_accessed=8 * 2**20, transcendentals=0),
        name="fetch",
    )(first, in_hbm(lengths), in_hbm(block_table[0]), k_hbm, v_hbm)
    query_all = lax.all_to_all(spread, "blk", split_axis=0, concat_axis=0, tiled=True)
    rows = SLICES * ROWS
    partial = pl.pallas_call(
        attend_kernel,
        out_shape=jax.ShapeDtypeStruct((devices, ROWS + 8, LANES), bf16),
        in_specs=[VMEM] * 4 + [HBM],
        out_specs=VMEM,
        scratch_shapes=[
            pltpu.VMEM((pool[0], (KVH - EARLY) * DH), bf16),
            pltpu.VMEM((2, rows, pool[0]), jnp.float32),
            pltpu.VMEM((2, rows, pool[0]), bf16),
            pltpu.VMEM((KVH, rows, LANES), jnp.float32),
            pltpu.VMEM((2, rows, LANES), jnp.float32),
            pltpu.SemaphoreType.DMA((KVH - EARLY,)),
        ],
        compiler_params=PARAMS,
        name="attend",
    )(bias, query_all, keys, values, v_hbm)
    collected = lax.all_to_all(partial, "blk", split_axis=0, concat_axis=0, tiled=True)
    return pl.pallas_call(
        combine_kernel,
        out_shape=jax.ShapeDtypeStruct((TOK, HEADS * DH), bf16),
        in_specs=[VMEM],
        out_specs=VMEM,
        compiler_params=PARAMS,
        name="combine",
    )(collected)


def solution(mesh):
    placed = (
        P(None, ("blk", "grp")),
        P("grp", "blk", None, None),
        P("grp", "blk", None, None),
        P("grp", None),
        P("grp", None, None),
    )
    return jax.shard_map(
        body, mesh=mesh, in_specs=placed, out_specs=P("grp", "blk"), check_vma=False
    )
```

```python
import math

import jax
import jax.numpy as jnp
from jax import lax
from jax.experimental import pallas as pl
from jax.experimental.pallas import tpu as pltpu
from jax.sharding import PartitionSpec as P

HQ = 64
KVH = 8
DH = 128
STEPS = 3
SEQS = 4
TOK = SEQS * STEPS
HEADS = 2
ROWS = HEADS * TOK
SLICES = 4
SLOTS = 8
WIDE = 256
CHUNK = 16
BLOCK = 128
FETCHES = 8
LATE = 6
EARLY = 4
LANES = 128
HALF_FEATS = 8
HALF = 16
SCALE = math.log2(math.e) / math.sqrt(DH)
LN2 = math.log(2.0)
EMPTY = -1e30

VMEM = pl.BlockSpec(memory_space=pltpu.VMEM)
HBM = pl.BlockSpec(memory_space=pltpu.HBM)
SMEM = pl.BlockSpec(memory_space=pltpu.SMEM)


PARAMS = pltpu.CompilerParams(vmem_limit_bytes=16 * 1024 * 1024)


def in_hbm(array):
    return pltpu.with_memory_space_constraint(array, pltpu.HBM)


def iota(shape, dim):
    return lax.broadcasted_iota(jnp.int32, shape, dim)


def pack_kernel(q_ref, out_ref):
    groups, feats, _ = out_ref.shape
    q = q_ref[...].astype(jnp.float32)
    lane = iota((feats, LANES), 1)
    wide = jnp.concatenate([q, jnp.zeros((2 * feats, 2 * LANES - q.shape[1]), jnp.float32)], axis=1)

    def turned(part, shift):
        shift %= 2 * LANES
        return (part if shift == 0 else pltpu.roll(part, shift, 1))[:, :LANES]

    for g in range(groups):
        low = turned(wide[:feats], -g * TOK)
        high = turned(wide[feats:], HALF - g * TOK)
        both = jnp.where(lane < TOK, low, jnp.where((lane >= HALF) & (lane < HALF + TOK), high, 0.0))
        out_ref[g] = both.astype(out_ref.dtype)


def spread_kernel(a_ref, out_ref):
    feats = a_ref.shape[0]
    row = iota((ROWS, LANES), 0)
    tok = jnp.where(row >= TOK, row - TOK, row)
    lane = iota((ROWS, LANES), 1)
    nt = (((1,), (1,)), ((), ()))
    nn = (((1,), (0,)), ((), ()))
    halves = []
    for j in range(2):
        pick = (lane == tok + j * HALF).astype(jnp.bfloat16)
        halves.append(lax.dot_general(pick, a_ref[...], nt, preferred_element_type=jnp.float32))
    apart = jnp.concatenate(halves, axis=1).astype(jnp.bfloat16)
    at = iota((2 * feats, 2 * feats), 0)
    to = iota((2 * feats, 2 * feats), 1)
    second = at >= feats
    at = jnp.where(second, at - feats, at)
    order = to == (at // HALF_FEATS) * (2 * HALF_FEATS) + at % HALF_FEATS + jnp.where(second, HALF_FEATS, 0)
    whole = lax.dot_general(
        apart, order.astype(jnp.bfloat16), nn, preferred_element_type=jnp.float32
    )
    rows = jnp.where(row < TOK, whole[:, :LANES], whole[:, LANES:]).astype(out_ref.dtype)
    for b in range(out_ref.shape[0]):
        out_ref[b] = rows


def fetch_kernel(
    first_ref, len_hbm, table_hbm, k_hbm, v_hbm,
    k_ref, v_ref, bias_ref, len_ref, table_ref, sems, small,
):
    rows = k_ref.shape[0] // FETCHES
    copies = []
    for i in range(FETCHES):
        at = pl.ds(i * rows, rows)
        copies.append(pltpu.make_async_copy(k_hbm.at[at], k_ref.at[at], sems.at[0, i]))
        copies.append(
            pltpu.make_async_copy(v_hbm.at[at, pl.ds(0, EARLY * DH)], v_ref.at[at], sems.at[1, i])
        )
    facts = [
        pltpu.make_async_copy(table_hbm, table_ref, small.at[0]),
        pltpu.make_async_copy(len_hbm, len_ref, small.at[1]),
    ]
    for c in facts + copies:
        c.start()
    for c in facts:
        c.wait()
    lane4 = iota((SEQS, LANES), 1)
    sub4 = iota((SEQS, LANES), 0)
    lens = jnp.zeros((SEQS, LANES), jnp.int32)
    for q in range(SEQS):
        lens = jnp.where(sub4 == q, len_ref[0, q], lens)
    local = jnp.where(lane4 < lens, table_ref[...] - first_ref[0], -1)
    row = iota((ROWS, LANES), 0)
    seq = jnp.where(row >= TOK, row - TOK, row) // STEPS
    for s in range(SLOTS):
        hit = jnp.max((local == s).astype(jnp.float32), axis=1, keepdims=True)
        off = jnp.broadcast_to(jnp.where(hit > 0.0, 0.0, EMPTY), (SEQS, LANES))
        b = jnp.broadcast_to(off[0:1], (ROWS, LANES))
        for q in range(1, SEQS):
            b = jnp.where(seq == q, off[q : q + 1], b)
        bias_ref[:, s * BLOCK : (s + 1) * BLOCK] = b
    for c in copies:
        c.wait()


def attend_kernel(
    bias_ref, q_ref, k_ref, v_ref, v_hbm, out_ref, late_ref, s_ref, p_ref, top_ref, sum_ref, sems
):
    def late(k):
        return pltpu.make_async_copy(
            v_hbm.at[:, pl.ds(pl.multiple_of((EARLY + k) * DH, DH), DH)],
            late_ref.at[:, pl.ds(pl.multiple_of(k * DH, DH), DH)],
            sems.at[k],
        )

    def send_for(k, carry):
        late(k).start()
        return carry

    lax.fori_loop(0, KVH - EARLY, send_for, 0)
    rows = SLICES * ROWS
    lane = iota((rows, LANES), 1)
    lse = jnp.zeros((rows, LANES), jnp.float32)
    nt = (((1,), (1,)), ((), ()))
    nn = (((1,), (0,)), ((), ()))

    def cols(k):
        return slice(k * DH, (k + 1) * DH)

    def scores(k):
        qk = q_ref[k * SLICES : (k + 1) * SLICES].reshape(rows, DH)
        most = None
        for j in range(0, SLOTS * BLOCK, WIDE):
            at = slice(j, j + WIDE)
            s = lax.dot_general(qk, k_ref[at, cols(k)], nt, preferred_element_type=jnp.float32)
            s = s + jnp.concatenate([bias_ref[:, at]] * SLICES, axis=0)
            s_ref[k % 2, :, at] = s
            for i in range(0, WIDE, LANES):
                part = s[:, i : i + LANES]
                most = part if most is None else jnp.maximum(most, part)
        top = jnp.max(most, axis=1, keepdims=True)
        top_ref[k] = jnp.broadcast_to(top, (rows, LANES))

    def weights(k, lse):
        for r in range(0, rows, CHUNK):
            at = slice(r, r + CHUNK)
            top = top_ref[k, at]
            total = None
            for j in range(0, SLOTS * BLOCK, LANES):
                here = slice(j, j + LANES)
                p = jnp.exp2((s_ref[k % 2, at, here] - top) * SCALE)
                total = p if total is None else total + p
                p_ref[k % 2, at, here] = p.astype(jnp.bfloat16)
            sum_ref[k % 2, at] = jnp.broadcast_to(
                jnp.sum(total, axis=1, keepdims=True), (CHUNK, LANES)
            )
        return jnp.where(lane == k, top_ref[k] * SCALE + jnp.log2(sum_ref[k % 2]), lse)

    def values(k):
        if k < EARLY:
            v = v_ref[:, cols(k)]
        else:
            v = late_ref[:, cols(k - EARLY)]
        o = lax.dot_general(p_ref[k % 2], v, nn, preferred_element_type=jnp.float32)
        o = (o * (1.0 / sum_ref[k % 2])).astype(out_ref.dtype)
        out_ref[k * SLICES : (k + 1) * SLICES, :ROWS, :] = o.reshape(SLICES, ROWS, DH)

    for step in range(KVH + 2):
        if step == LATE:
            for k in range(KVH - EARLY):
                late(k).wait()
        if step < KVH:
            scores(step)
        if 0 <= step - 1 < KVH:
            lse = weights(step - 1, lse)
        if step >= 2:
            values(step - 2)
    square = jnp.concatenate([lse, jnp.zeros((LANES - rows, LANES), jnp.float32)], axis=0)
    flat = jnp.transpose(square)[:KVH]
    lane8 = iota((KVH, LANES), 1)
    for j in range(SLICES):
        mine = flat if j == 0 else pltpu.roll(flat, LANES - j * ROWS, 1)
        mine = jnp.where(lane8 < ROWS, mine, 0.0)
        high = mine.astype(jnp.bfloat16).astype(jnp.float32)
        rest = mine - high
        mid = rest.astype(jnp.bfloat16).astype(jnp.float32)
        low = rest - mid
        line = high + pltpu.roll(mid, 32, 1) + pltpu.roll(low, 64, 1)
        for k in range(KVH):
            tile = jnp.broadcast_to(line[k : k + 1], (8, LANES))
            out_ref[k * SLICES + j, ROWS:, :] = tile.astype(out_ref.dtype)


def combine_kernel(a_ref, out_ref):
    devices = a_ref.shape[0]
    sub8 = iota((8, LANES), 0)
    parts = []
    for t in range(devices // 8):
        acc = a_ref[8 * t, ROWS:, :].astype(jnp.float32)
        for j in range(1, 8):
            acc = jnp.where(sub8 == j, a_ref[8 * t + j, ROWS:, :].astype(jnp.float32), acc)
        parts.append(acc)
    stat = jnp.concatenate(parts, axis=0)
    lse = stat + pltpu.roll(stat, LANES - 32, 1) + pltpu.roll(stat, LANES - 64, 1)
    top = jnp.max(lse, axis=0, keepdims=True)
    w = jnp.exp2(lse - top)
    w = w / jnp.sum(w, axis=0, keepdims=True)
    square = jnp.concatenate([w, jnp.zeros((LANES - devices, LANES), jnp.float32)], axis=0)
    wt = jnp.transpose(square)[:ROWS]
    acc = jnp.zeros((ROWS, LANES), jnp.float32)
    for b in range(devices):
        acc = acc + wt[:, b : b + 1] * a_ref[b, :ROWS, :].astype(jnp.float32)
    out_ref[...] = jnp.concatenate([acc[:TOK], acc[TOK:]], axis=1).astype(out_ref.dtype)


def body(queries, key_pool, value_pool, lengths, block_table):
    bf16 = jnp.bfloat16
    groups = lax.axis_size("grp")
    devices = lax.axis_size("blk")
    first = (lax.axis_index("blk") * SLOTS).astype(jnp.int32).reshape(1)
    packed = pl.pallas_call(
        pack_kernel,
        out_shape=jax.ShapeDtypeStruct((groups, HALF_FEATS, LANES), bf16),
        in_specs=[VMEM],
        out_specs=VMEM,
        compiler_params=PARAMS,
        name="pack",
    )(queries.T)
    arrived = lax.all_to_all(packed, "grp", split_axis=0, concat_axis=0, tiled=True)
    spread = pl.pallas_call(
        spread_kernel,
        out_shape=jax.ShapeDtypeStruct((devices, ROWS, LANES), bf16),
        in_specs=[VMEM],
        out_specs=VMEM,
        compiler_params=PARAMS,
        name="spread",
    )(arrived.reshape(groups * HALF_FEATS, LANES))
    pool = (SLOTS * BLOCK, KVH * DH)
    k_hbm = in_hbm(key_pool.reshape(pool))
    v_hbm = in_hbm(value_pool.reshape(pool))
    keys, values, bias = pl.pallas_call(
        fetch_kernel,
        out_shape=(
            pltpu.VMEM(pool, bf16),
            pltpu.VMEM((pool[0], EARLY * DH), bf16),
            pltpu.VMEM((ROWS, pool[0]), jnp.float32),
        ),
        in_specs=[SMEM, HBM, HBM, HBM, HBM],
        out_specs=(VMEM,) * 3,
        scratch_shapes=[
            pltpu.SMEM(lengths.shape, jnp.int32),
            pltpu.VMEM(block_table.shape[1:], jnp.int32),
            pltpu.SemaphoreType.DMA((2, FETCHES)),
            pltpu.SemaphoreType.DMA((2,)),
        ],
        compiler_params=PARAMS,
        cost_estimate=pl.CostEstimate(flops=10**9, bytes_accessed=8 * 2**20, transcendentals=0),
        name="fetch",
    )(first, in_hbm(lengths), in_hbm(block_table[0]), k_hbm, v_hbm)
    query_all = lax.all_to_all(spread, "blk", split_axis=0, concat_axis=0, tiled=True)
    rows = SLICES * ROWS
    partial = pl.pallas_call(
        attend_kernel,
        out_shape=jax.ShapeDtypeStruct((devices, ROWS + 8, LANES), bf16),
        in_specs=[VMEM] * 4 + [HBM],
        out_specs=VMEM,
        scratch_shapes=[
            pltpu.VMEM((pool[0], (KVH - EARLY) * DH), bf16),
            pltpu.VMEM((2, rows, pool[0]), jnp.float32),
            pltpu.VMEM((2, rows, pool[0]), bf16),
            pltpu.VMEM((KVH, rows, LANES), jnp.float32),
            pltpu.VMEM((2, rows, LANES), jnp.float32),
            pltpu.SemaphoreType.DMA((KVH - EARLY,)),
        ],
        compiler_params=PARAMS,
        name="attend",
    )(bias, query_all, keys, values, v_hbm)
    collected = lax.all_to_all(partial, "blk", split_axis=0, concat_axis=0, tiled=True)
    return pl.pallas_call(
        combine_kernel,
        out_shape=jax.ShapeDtypeStruct((TOK, HEADS * DH), bf16),
        in_specs=[VMEM],
        out_specs=VMEM,
        compiler_params=PARAMS,
        name="combine",
    )(collected)


def solution(mesh):
    placed = (
        P(None, ("blk", "grp")),
        P("grp", "blk", None, None),
        P("grp", "blk", None, None),
        P("grp", None),
        P("grp", None, None),
    )
    return jax.shard_map(
        body, mesh=mesh, in_specs=placed, out_specs=P("grp", "blk"), check_vma=False
    )
```

```python
import math

import jax
import jax.numpy as jnp
from jax import lax
from jax.experimental import pallas as pl
from jax.experimental.pallas import tpu as pltpu
from jax.sharding import PartitionSpec as P

HQ = 64
KVH = 8
DH = 128
STEPS = 3
SEQS = 4
TOK = SEQS * STEPS
HEADS = 2
ROWS = HEADS * TOK
SLICES = 4
SLOTS = 8
WIDE = 256
CHUNK = 16
BLOCK = 128
FETCHES = 8
LATE = 6
EARLY = 4
LANES = 128
HALF_FEATS = 8
HALF = 16
SCALE = math.log2(math.e) / math.sqrt(DH)
LN2 = math.log(2.0)
EMPTY = -1e30

SIDE_X, SIDE_Y = 4, 8
WALK = [
    (x if y % 2 == 0 else SIDE_X - 1 - x) * SIDE_Y + y for y in range(SIDE_Y) for x in range(SIDE_X)
]
STAND = [WALK.index(b) for b in range(len(WALK))]

VMEM = pl.BlockSpec(memory_space=pltpu.VMEM)
HBM = pl.BlockSpec(memory_space=pltpu.HBM)
SMEM = pl.BlockSpec(memory_space=pltpu.SMEM)


PARAMS = pltpu.CompilerParams(vmem_limit_bytes=16 * 1024 * 1024)


def in_hbm(array):
    return pltpu.with_memory_space_constraint(array, pltpu.HBM)


def iota(shape, dim):
    return lax.broadcasted_iota(jnp.int32, shape, dim)


def pack_kernel(q_ref, out_ref):
    groups, feats, _ = out_ref.shape
    q = q_ref[...].astype(jnp.float32)
    lane = iota((feats, LANES), 1)
    wide = jnp.concatenate([q, jnp.zeros((2 * feats, 2 * LANES - q.shape[1]), jnp.float32)], axis=1)

    def turned(part, shift):
        shift %= 2 * LANES
        return (part if shift == 0 else pltpu.roll(part, shift, 1))[:, :LANES]

    for g in range(groups):
        low = turned(wide[:feats], -g * TOK)
        high = turned(wide[feats:], HALF - g * TOK)
        both = jnp.where(lane < TOK, low, jnp.where((lane >= HALF) & (lane < HALF + TOK), high, 0.0))
        out_ref[g] = both.astype(out_ref.dtype)


def spread_kernel(a_ref, out_ref):
    feats = a_ref.shape[0]
    row = iota((ROWS, LANES), 0)
    tok = jnp.where(row >= TOK, row - TOK, row)
    lane = iota((ROWS, LANES), 1)
    nt = (((1,), (1,)), ((), ()))
    nn = (((1,), (0,)), ((), ()))
    halves = []
    for j in range(2):
        pick = (lane == tok + j * HALF).astype(jnp.bfloat16)
        halves.append(lax.dot_general(pick, a_ref[...], nt, preferred_element_type=jnp.float32))
    apart = jnp.concatenate(halves, axis=1).astype(jnp.bfloat16)
    at = iota((2 * feats, 2 * feats), 0)
    to = iota((2 * feats, 2 * feats), 1)
    second = at >= feats
    at = jnp.where(second, at - feats, at)
    order = to == (at // HALF_FEATS) * (2 * HALF_FEATS) + at % HALF_FEATS + jnp.where(second, HALF_FEATS, 0)
    whole = lax.dot_general(
        apart, order.astype(jnp.bfloat16), nn, preferred_element_type=jnp.float32
    )
    rows = jnp.where(row < TOK, whole[:, :LANES], whole[:, LANES:]).astype(out_ref.dtype)
    for b in range(out_ref.shape[0]):
        out_ref[b] = rows


def fetch_kernel(
    first_ref, len_hbm, table_hbm, k_hbm, v_hbm,
    k_ref, v_ref, bias_ref, len_ref, table_ref, sems, small,
):
    rows = k_ref.shape[0] // FETCHES
    copies = []
    for i in range(FETCHES):
        at = pl.ds(i * rows, rows)
        copies.append(pltpu.make_async_copy(k_hbm.at[at], k_ref.at[at], sems.at[0, i]))
        copies.append(
            pltpu.make_async_copy(v_hbm.at[at, pl.ds(0, EARLY * DH)], v_ref.at[at], sems.at[1, i])
        )
    facts = [
        pltpu.make_async_copy(table_hbm, table_ref, small.at[0]),
        pltpu.make_async_copy(len_hbm, len_ref, small.at[1]),
    ]
    for c in facts + copies:
        c.start()
    for c in facts:
        c.wait()
    lane4 = iota((SEQS, LANES), 1)
    sub4 = iota((SEQS, LANES), 0)
    lens = jnp.zeros((SEQS, LANES), jnp.int32)
    for q in range(SEQS):
        lens = jnp.where(sub4 == q, len_ref[0, q], lens)
    local = jnp.where(lane4 < lens, table_ref[...] - first_ref[0], -1)
    row = iota((ROWS, LANES), 0)
    seq = jnp.where(row >= TOK, row - TOK, row) // STEPS
    for s in range(SLOTS):
        hit = jnp.max((local == s).astype(jnp.float32), axis=1, keepdims=True)
        off = jnp.broadcast_to(jnp.where(hit > 0.0, 0.0, EMPTY), (SEQS, LANES))
        b = jnp.broadcast_to(off[0:1], (ROWS, LANES))
        for q in range(1, SEQS):
            b = jnp.where(seq == q, off[q : q + 1], b)
        bias_ref[:, s * BLOCK : (s + 1) * BLOCK] = b
    for c in copies:
        c.wait()


def attend_kernel(
    bias_ref, q_ref, k_ref, v_ref, v_hbm, out_ref, late_ref, s_ref, p_ref, top_ref, sum_ref, sems
):
    def late(k):
        return pltpu.make_async_copy(
            v_hbm.at[:, pl.ds(pl.multiple_of((EARLY + k) * DH, DH), DH)],
            late_ref.at[:, pl.ds(pl.multiple_of(k * DH, DH), DH)],
            sems.at[k],
        )

    def send_for(k, carry):
        late(k).start()
        return carry

    lax.fori_loop(0, KVH - EARLY, send_for, 0)
    rows = SLICES * ROWS
    lane = iota((rows, LANES), 1)
    lse = jnp.zeros((rows, LANES), jnp.float32)
    nt = (((1,), (1,)), ((), ()))
    nn = (((1,), (0,)), ((), ()))

    def cols(k):
        return slice(k * DH, (k + 1) * DH)

    def scores(k):
        qk = jnp.concatenate([q_ref[STAND[k * SLICES + j]] for j in range(SLICES)], axis=0)
        most = None
        for j in range(0, SLOTS * BLOCK, WIDE):
            at = slice(j, j + WIDE)
            s = lax.dot_general(qk, k_ref[at, cols(k)], nt, preferred_element_type=jnp.float32)
            s = s + jnp.concatenate([bias_ref[:, at]] * SLICES, axis=0)
            s_ref[k % 2, :, at] = s
            for i in range(0, WIDE, LANES):
                part = s[:, i : i + LANES]
                most = part if most is None else jnp.maximum(most, part)
        top = jnp.max(most, axis=1, keepdims=True)
        top_ref[k] = jnp.broadcast_to(top, (rows, LANES))

    def weights(k, lse):
        for r in range(0, rows, CHUNK):
            at = slice(r, r + CHUNK)
            top = top_ref[k, at]
            total = None
            for j in range(0, SLOTS * BLOCK, LANES):
                here = slice(j, j + LANES)
                p = jnp.exp2((s_ref[k % 2, at, here] - top) * SCALE)
                total = p if total is None else total + p
                p_ref[k % 2, at, here] = p.astype(jnp.bfloat16)
            sum_ref[k % 2, at] = jnp.broadcast_to(
                jnp.sum(total, axis=1, keepdims=True), (CHUNK, LANES)
            )
        return jnp.where(lane == k, top_ref[k] * SCALE + jnp.log2(sum_ref[k % 2]), lse)

    def values(k):
        if k < EARLY:
            v = v_ref[:, cols(k)]
        else:
            v = late_ref[:, cols(k - EARLY)]
        o = lax.dot_general(p_ref[k % 2], v, nn, preferred_element_type=jnp.float32)
        o = (o * (1.0 / sum_ref[k % 2])).astype(out_ref.dtype)
        for j in range(SLICES):
            out_ref[STAND[k * SLICES + j], :ROWS, :] = o[j * ROWS : (j + 1) * ROWS]

    for step in range(KVH + 2):
        if step == LATE:
            for k in range(KVH - EARLY):
                late(k).wait()
        if step < KVH:
            scores(step)
        if 0 <= step - 1 < KVH:
            lse = weights(step - 1, lse)
        if step >= 2:
            values(step - 2)
    square = jnp.concatenate([lse, jnp.zeros((LANES - rows, LANES), jnp.float32)], axis=0)
    flat = jnp.transpose(square)[:KVH]
    lane8 = iota((KVH, LANES), 1)
    for j in range(SLICES):
        mine = flat if j == 0 else pltpu.roll(flat, LANES - j * ROWS, 1)
        mine = jnp.where(lane8 < ROWS, mine, 0.0)
        high = mine.astype(jnp.bfloat16).astype(jnp.float32)
        rest = mine - high
        mid = rest.astype(jnp.bfloat16).astype(jnp.float32)
        low = rest - mid
        line = high + pltpu.roll(mid, 32, 1) + pltpu.roll(low, 64, 1)
        for k in range(KVH):
            tile = jnp.broadcast_to(line[k : k + 1], (8, LANES))
            out_ref[STAND[k * SLICES + j], ROWS:, :] = tile.astype(out_ref.dtype)


def combine_kernel(a_ref, out_ref):
    devices = a_ref.shape[0]
    sub8 = iota((8, LANES), 0)
    parts = []
    for t in range(devices // 8):
        acc = a_ref[8 * t, ROWS:, :].astype(jnp.float32)
        for j in range(1, 8):
            acc = jnp.where(sub8 == j, a_ref[8 * t + j, ROWS:, :].astype(jnp.float32), acc)
        parts.append(acc)
    stat = jnp.concatenate(parts, axis=0)
    lse = stat + pltpu.roll(stat, LANES - 32, 1) + pltpu.roll(stat, LANES - 64, 1)
    top = jnp.max(lse, axis=0, keepdims=True)
    w = jnp.exp2(lse - top)
    w = w / jnp.sum(w, axis=0, keepdims=True)
    square = jnp.concatenate([w, jnp.zeros((LANES - devices, LANES), jnp.float32)], axis=0)
    wt = jnp.transpose(square)[:ROWS]
    acc = jnp.zeros((ROWS, LANES), jnp.float32)
    for b in range(devices):
        acc = acc + wt[:, b : b + 1] * a_ref[b, :ROWS, :].astype(jnp.float32)
    out_ref[...] = jnp.concatenate([acc[:TOK], acc[TOK:]], axis=1).astype(out_ref.dtype)


def exchange(pieces):
    return lax.all_to_all(
        pieces, "blk", split_axis=0, concat_axis=0, tiled=True, axis_index_groups=[WALK]
    )


def body(queries, key_pool, value_pool, lengths, block_table):
    bf16 = jnp.bfloat16
    groups = lax.axis_size("grp")
    devices = lax.axis_size("blk")
    first = (lax.axis_index("blk") * SLOTS).astype(jnp.int32).reshape(1)
    packed = pl.pallas_call(
        pack_kernel,
        out_shape=jax.ShapeDtypeStruct((groups, HALF_FEATS, LANES), bf16),
        in_specs=[VMEM],
        out_specs=VMEM,
        compiler_params=PARAMS,
        name="pack",
    )(queries.T)
    arrived = lax.all_to_all(packed, "grp", split_axis=0, concat_axis=0, tiled=True)
    spread = pl.pallas_call(
        spread_kernel,
        out_shape=jax.ShapeDtypeStruct((devices, ROWS, LANES), bf16),
        in_specs=[VMEM],
        out_specs=VMEM,
        compiler_params=PARAMS,
        name="spread",
    )(arrived.reshape(groups * HALF_FEATS, LANES))
    pool = (SLOTS * BLOCK, KVH * DH)
    k_hbm = in_hbm(key_pool.reshape(pool))
    v_hbm = in_hbm(value_pool.reshape(pool))
    keys, values, bias = pl.pallas_call(
        fetch_kernel,
        out_shape=(
            pltpu.VMEM(pool, bf16),
            pltpu.VMEM((pool[0], EARLY * DH), bf16),
            pltpu.VMEM((ROWS, pool[0]), jnp.float32),
        ),
        in_specs=[SMEM, HBM, HBM, HBM, HBM],
        out_specs=(VMEM,) * 3,
        scratch_shapes=[
            pltpu.SMEM(lengths.shape, jnp.int32),
            pltpu.VMEM(block_table.shape[1:], jnp.int32),
            pltpu.SemaphoreType.DMA((2, FETCHES)),
            pltpu.SemaphoreType.DMA((2,)),
        ],
        compiler_params=PARAMS,
        cost_estimate=pl.CostEstimate(flops=10**9, bytes_accessed=8 * 2**20, transcendentals=0),
        name="fetch",
    )(first, in_hbm(lengths), in_hbm(block_table[0]), k_hbm, v_hbm)
    query_all = exchange(spread)
    rows = SLICES * ROWS
    partial = pl.pallas_call(
        attend_kernel,
        out_shape=jax.ShapeDtypeStruct((devices, ROWS + 8, LANES), bf16),
        in_specs=[VMEM] * 4 + [HBM],
        out_specs=VMEM,
        scratch_shapes=[
            pltpu.VMEM((pool[0], (KVH - EARLY) * DH), bf16),
            pltpu.VMEM((2, rows, pool[0]), jnp.float32),
            pltpu.VMEM((2, rows, pool[0]), bf16),
            pltpu.VMEM((KVH, rows, LANES), jnp.float32),
            pltpu.VMEM((2, rows, LANES), jnp.float32),
            pltpu.SemaphoreType.DMA((KVH - EARLY,)),
        ],
        compiler_params=PARAMS,
        name="attend",
    )(bias, query_all, keys, values, v_hbm)
    collected = exchange(partial)
    return pl.pallas_call(
        combine_kernel,
        out_shape=jax.ShapeDtypeStruct((TOK, HEADS * DH), bf16),
        in_specs=[VMEM],
        out_specs=VMEM,
        compiler_params=PARAMS,
        name="combine",
    )(collected)


def solution(mesh):
    placed = (
        P(None, ("blk", "grp")),
        P("grp", "blk", None, None),
        P("grp", "blk", None, None),
        P("grp", None),
        P("grp", None, None),
    )
    return jax.shard_map(
        body, mesh=mesh, in_specs=placed, out_specs=P("grp", "blk"), check_vma=False
    )
```

```python
import math

import jax
import jax.numpy as jnp
from jax import lax
from jax.experimental import pallas as pl
from jax.experimental.pallas import tpu as pltpu
from jax.sharding import PartitionSpec as P

HQ = 64
KVH = 8
DH = 128
STEPS = 3
SEQS = 4
TOK = SEQS * STEPS
HEADS = 2
ROWS = HEADS * TOK
SLICES = 4
SLOTS = 8
WIDE = 256
CHUNK = 16
BLOCK = 128
FETCHES = 8
LATE = 6
EARLY = 4
LANES = 128
HALF_FEATS = 8
HALF = 16
SCALE = math.log2(math.e) / math.sqrt(DH)
LN2 = math.log(2.0)
EMPTY = -1e30

SIDE_X, SIDE_Y = 4, 8
WALK = [
    (x if y % 2 == 0 else SIDE_X - 1 - x) * SIDE_Y + y for y in range(SIDE_Y) for x in range(SIDE_X)
]
STAND = [WALK.index(b) for b in range(len(WALK))]

VMEM = pl.BlockSpec(memory_space=pltpu.VMEM)
HBM = pl.BlockSpec(memory_space=pltpu.HBM)
SMEM = pl.BlockSpec(memory_space=pltpu.SMEM)


PARAMS = pltpu.CompilerParams(vmem_limit_bytes=16 * 1024 * 1024)


def in_hbm(array):
    return pltpu.with_memory_space_constraint(array, pltpu.HBM)


def iota(shape, dim):
    return lax.broadcasted_iota(jnp.int32, shape, dim)


def pack_kernel(q_ref, out_ref):
    groups, feats, _ = out_ref.shape
    q = q_ref[...].astype(jnp.float32)
    lane = iota((feats, LANES), 1)
    wide = jnp.concatenate([q, jnp.zeros((2 * feats, 2 * LANES - q.shape[1]), jnp.float32)], axis=1)

    def turned(part, shift):
        shift %= 2 * LANES
        return (part if shift == 0 else pltpu.roll(part, shift, 1))[:, :LANES]

    for g in range(groups):
        low = turned(wide[:feats], -g * TOK)
        high = turned(wide[feats:], HALF - g * TOK)
        both = jnp.where(lane < TOK, low, jnp.where((lane >= HALF) & (lane < HALF + TOK), high, 0.0))
        out_ref[g] = both.astype(out_ref.dtype)


def spread_kernel(a_ref, out_ref):
    feats = a_ref.shape[0]
    row = iota((ROWS, LANES), 0)
    tok = jnp.where(row >= TOK, row - TOK, row)
    lane = iota((ROWS, LANES), 1)
    nt = (((1,), (1,)), ((), ()))
    tiles = [a_ref[g : g + HALF_FEATS] for g in range(0, feats, HALF_FEATS)]
    twice = jnp.concatenate([t for t in tiles for _ in range(2)], axis=0)
    pick = jnp.concatenate([lane == tok, lane == tok + HALF], axis=0).astype(jnp.bfloat16)
    both = lax.dot_general(pick, twice, nt, preferred_element_type=jnp.float32)
    odd = (iota((ROWS, 2 * feats), 1) // HALF_FEATS) % 2 == 1
    whole = jnp.where(odd, both[ROWS:], both[:ROWS])
    rows = jnp.where(row < TOK, whole[:, :LANES], whole[:, LANES:]).astype(out_ref.dtype)
    for b in range(out_ref.shape[0]):
        out_ref[b] = rows


def fetch_kernel(
    first_ref, len_hbm, table_hbm, k_hbm, v_hbm,
    k_ref, v_ref, bias_ref, len_ref, table_ref, sems, small,
):
    rows = k_ref.shape[0] // FETCHES
    copies = []
    for i in range(FETCHES):
        at = pl.ds(i * rows, rows)
        copies.append(pltpu.make_async_copy(k_hbm.at[at], k_ref.at[at], sems.at[0, i]))
        copies.append(
            pltpu.make_async_copy(v_hbm.at[at, pl.ds(0, EARLY * DH)], v_ref.at[at], sems.at[1, i])
        )
    facts = [
        pltpu.make_async_copy(table_hbm, table_ref, small.at[0]),
        pltpu.make_async_copy(len_hbm, len_ref, small.at[1]),
    ]
    for c in facts + copies:
        c.start()
    for c in facts:
        c.wait()
    lane4 = iota((SEQS, LANES), 1)
    sub4 = iota((SEQS, LANES), 0)
    lens = jnp.zeros((SEQS, LANES), jnp.int32)
    for q in range(SEQS):
        lens = jnp.where(sub4 == q, len_ref[0, q], lens)
    local = jnp.where(lane4 < lens, table_ref[...] - first_ref[0], -1)
    row = iota((ROWS, LANES), 0)
    seq = jnp.where(row >= TOK, row - TOK, row) // STEPS
    for s in range(SLOTS):
        hit = jnp.max((local == s).astype(jnp.float32), axis=1, keepdims=True)
        off = jnp.broadcast_to(jnp.where(hit > 0.0, 0.0, EMPTY), (SEQS, LANES))
        b = jnp.broadcast_to(off[0:1], (ROWS, LANES))
        for q in range(1, SEQS):
            b = jnp.where(seq == q, off[q : q + 1], b)
        bias_ref[:, s * BLOCK : (s + 1) * BLOCK] = b
    for c in copies:
        c.wait()


def attend_kernel(
    bias_ref, q_ref, k_ref, v_ref, v_hbm, out_ref, late_ref, s_ref, p_ref, top_ref, sum_ref, sems
):
    def late(k):
        return pltpu.make_async_copy(
            v_hbm.at[:, pl.ds(pl.multiple_of((EARLY + k) * DH, DH), DH)],
            late_ref.at[:, pl.ds(pl.multiple_of(k * DH, DH), DH)],
            sems.at[k],
        )

    def send_for(k, carry):
        late(k).start()
        return carry

    lax.fori_loop(0, KVH - EARLY, send_for, 0)
    rows = SLICES * ROWS
    lane = iota((rows, LANES), 1)
    lse = jnp.zeros((rows, LANES), jnp.float32)
    nt = (((1,), (1,)), ((), ()))
    nn = (((1,), (0,)), ((), ()))

    def cols(k):
        return slice(k * DH, (k + 1) * DH)

    def scores(k):
        qk = jnp.concatenate([q_ref[STAND[k * SLICES + j]] for j in range(SLICES)], axis=0)
        most = None
        for j in range(0, SLOTS * BLOCK, WIDE):
            at = slice(j, j + WIDE)
            s = lax.dot_general(qk, k_ref[at, cols(k)], nt, preferred_element_type=jnp.float32)
            s = s + jnp.concatenate([bias_ref[:, at]] * SLICES, axis=0)
            s_ref[k % 2, :, at] = s
            for i in range(0, WIDE, LANES):
                part = s[:, i : i + LANES]
                most = part if most is None else jnp.maximum(most, part)
        top = jnp.max(most, axis=1, keepdims=True)
        top_ref[k] = jnp.broadcast_to(top, (rows, LANES))

    def weights(k, lse):
        for r in range(0, rows, CHUNK):
            at = slice(r, r + CHUNK)
            top = top_ref[k, at]
            total = None
            for j in range(0, SLOTS * BLOCK, LANES):
                here = slice(j, j + LANES)
                p = jnp.exp2((s_ref[k % 2, at, here] - top) * SCALE)
                total = p if total is None else total + p
                p_ref[k % 2, at, here] = p.astype(jnp.bfloat16)
            sum_ref[k % 2, at] = jnp.broadcast_to(
                jnp.sum(total, axis=1, keepdims=True), (CHUNK, LANES)
            )
        return jnp.where(lane == k, top_ref[k] * SCALE + jnp.log2(sum_ref[k % 2]), lse)

    def values(k):
        if k < EARLY:
            v = v_ref[:, cols(k)]
        else:
            v = late_ref[:, cols(k - EARLY)]
        o = lax.dot_general(p_ref[k % 2], v, nn, preferred_element_type=jnp.float32)
        o = (o * (1.0 / sum_ref[k % 2])).astype(out_ref.dtype)
        for j in range(SLICES):
            out_ref[STAND[k * SLICES + j], :ROWS, :] = o[j * ROWS : (j + 1) * ROWS]

    for step in range(KVH + 2):
        if step == LATE:
            for k in range(KVH - EARLY):
                late(k).wait()
        if step < KVH:
            scores(step)
        if 0 <= step - 1 < KVH:
            lse = weights(step - 1, lse)
        if step >= 2:
            values(step - 2)
    square = jnp.concatenate([lse, jnp.zeros((LANES - rows, LANES), jnp.float32)], axis=0)
    flat = jnp.transpose(square)[:KVH]
    lane8 = iota((KVH, LANES), 1)
    for j in range(SLICES):
        mine = flat if j == 0 else pltpu.roll(flat, LANES - j * ROWS, 1)
        mine = jnp.where(lane8 < ROWS, mine, 0.0)
        high = mine.astype(jnp.bfloat16).astype(jnp.float32)
        rest = mine - high
        mid = rest.astype(jnp.bfloat16).astype(jnp.float32)
        low = rest - mid
        line = high + pltpu.roll(mid, 32, 1) + pltpu.roll(low, 64, 1)
        for k in range(KVH):
            tile = jnp.broadcast_to(line[k : k + 1], (8, LANES))
            out_ref[STAND[k * SLICES + j], ROWS:, :] = tile.astype(out_ref.dtype)


def combine_kernel(a_ref, out_ref):
    devices = a_ref.shape[0]
    sub8 = iota((8, LANES), 0)
    parts = []
    for t in range(devices // 8):
        acc = a_ref[8 * t, ROWS:, :].astype(jnp.float32)
        for j in range(1, 8):
            acc = jnp.where(sub8 == j, a_ref[8 * t + j, ROWS:, :].astype(jnp.float32), acc)
        parts.append(acc)
    stat = jnp.concatenate(parts, axis=0)
    lse = stat + pltpu.roll(stat, LANES - 32, 1) + pltpu.roll(stat, LANES - 64, 1)
    top = jnp.max(lse, axis=0, keepdims=True)
    w = jnp.exp2(lse - top)
    w = w / jnp.sum(w, axis=0, keepdims=True)
    square = jnp.concatenate([w, jnp.zeros((LANES - devices, LANES), jnp.float32)], axis=0)
    wt = jnp.transpose(square)[:ROWS]
    acc = jnp.zeros((ROWS, LANES), jnp.float32)
    for b in range(devices):
        acc = acc + wt[:, b : b + 1] * a_ref[b, :ROWS, :].astype(jnp.float32)
    out_ref[...] = jnp.concatenate([acc[:TOK], acc[TOK:]], axis=1).astype(out_ref.dtype)


def exchange(pieces):
    return lax.all_to_all(
        pieces, "blk", split_axis=0, concat_axis=0, tiled=True, axis_index_groups=[WALK]
    )


def body(queries, key_pool, value_pool, lengths, block_table):
    bf16 = jnp.bfloat16
    groups = lax.axis_size("grp")
    devices = lax.axis_size("blk")
    first = (lax.axis_index("blk") * SLOTS).astype(jnp.int32).reshape(1)
    packed = pl.pallas_call(
        pack_kernel,
        out_shape=jax.ShapeDtypeStruct((groups, HALF_FEATS, LANES), bf16),
        in_specs=[VMEM],
        out_specs=VMEM,
        compiler_params=PARAMS,
        name="pack",
    )(queries.T)
    arrived = lax.all_to_all(packed, "grp", split_axis=0, concat_axis=0, tiled=True)
    spread = pl.pallas_call(
        spread_kernel,
        out_shape=jax.ShapeDtypeStruct((devices, ROWS, LANES), bf16),
        in_specs=[VMEM],
        out_specs=VMEM,
        compiler_params=PARAMS,
        name="spread",
    )(arrived.reshape(groups * HALF_FEATS, LANES))
    pool = (SLOTS * BLOCK, KVH * DH)
    k_hbm = in_hbm(key_pool.reshape(pool))
    v_hbm = in_hbm(value_pool.reshape(pool))
    keys, values, bias = pl.pallas_call(
        fetch_kernel,
        out_shape=(
            pltpu.VMEM(pool, bf16),
            pltpu.VMEM((pool[0], EARLY * DH), bf16),
            pltpu.VMEM((ROWS, pool[0]), jnp.float32),
        ),
        in_specs=[SMEM, HBM, HBM, HBM, HBM],
        out_specs=(VMEM,) * 3,
        scratch_shapes=[
            pltpu.SMEM(lengths.shape, jnp.int32),
            pltpu.VMEM(block_table.shape[1:], jnp.int32),
            pltpu.SemaphoreType.DMA((2, FETCHES)),
            pltpu.SemaphoreType.DMA((2,)),
        ],
        compiler_params=PARAMS,
        cost_estimate=pl.CostEstimate(flops=10**9, bytes_accessed=8 * 2**20, transcendentals=0),
        name="fetch",
    )(first, in_hbm(lengths), in_hbm(block_table[0]), k_hbm, v_hbm)
    query_all = exchange(spread)
    rows = SLICES * ROWS
    partial = pl.pallas_call(
        attend_kernel,
        out_shape=jax.ShapeDtypeStruct((devices, ROWS + 8, LANES), bf16),
        in_specs=[VMEM] * 4 + [HBM],
        out_specs=VMEM,
        scratch_shapes=[
            pltpu.VMEM((pool[0], (KVH - EARLY) * DH), bf16),
            pltpu.VMEM((2, rows, pool[0]), jnp.float32),
            pltpu.VMEM((2, rows, pool[0]), bf16),
            pltpu.VMEM((KVH, rows, LANES), jnp.float32),
            pltpu.VMEM((2, rows, LANES), jnp.float32),
            pltpu.SemaphoreType.DMA((KVH - EARLY,)),
        ],
        compiler_params=PARAMS,
        name="attend",
    )(bias, query_all, keys, values, v_hbm)
    collected = exchange(partial)
    return pl.pallas_call(
        combine_kernel,
        out_shape=jax.ShapeDtypeStruct((TOK, HEADS * DH), bf16),
        in_specs=[VMEM],
        out_specs=VMEM,
        compiler_params=PARAMS,
        name="combine",
    )(collected)


def solution(mesh):
    placed = (
        P(None, ("blk", "grp")),
        P("grp", "blk", None, None),
        P("grp", "blk", None, None),
        P("grp", None),
        P("grp", None, None),
    )
    return jax.shard_map(
        body, mesh=mesh, in_specs=placed, out_specs=P("grp", "blk"), check_vma=False
    )
```

```python
import math

import jax
import jax.numpy as jnp
from jax import lax
from jax.experimental import pallas as pl
from jax.experimental.pallas import tpu as pltpu
from jax.sharding import PartitionSpec as P

HQ = 64
KVH = 8
DH = 128
STEPS = 3
SEQS = 4
TOK = SEQS * STEPS
HEADS = 2
ROWS = HEADS * TOK
SLICES = 4
SLOTS = 8
WIDE = 256
CHUNK = 16
BLOCK = 128
LANES = 128
HALF_FEATS = 8
HALF = 16
SCALE = math.log2(math.e) / math.sqrt(DH)
LN2 = math.log(2.0)
EMPTY = -1e30

SIDE_X, SIDE_Y = 4, 8
WALK = [
    (x if y % 2 == 0 else SIDE_X - 1 - x) * SIDE_Y + y for y in range(SIDE_Y) for x in range(SIDE_X)
]
STAND = [WALK.index(b) for b in range(len(WALK))]

VMEM = pl.BlockSpec(memory_space=pltpu.VMEM)
HBM = pl.BlockSpec(memory_space=pltpu.HBM)
SMEM = pl.BlockSpec(memory_space=pltpu.SMEM)


LONG = pl.CostEstimate(flops=10**10, bytes_accessed=10**8, transcendentals=10**6)
PARAMS = pltpu.CompilerParams(vmem_limit_bytes=16 * 1024 * 1024)


def in_hbm(array):
    return pltpu.with_memory_space_constraint(array, pltpu.HBM)


def iota(shape, dim):
    return lax.broadcasted_iota(jnp.int32, shape, dim)


def pack_kernel(
    first_ref, len_hbm, table_hbm, q_hbm, out_ref, bias_ref, len_ref, table_ref, q_ref, sems
):
    copies = [
        pltpu.make_async_copy(q_hbm, q_ref, sems.at[0]),
        pltpu.make_async_copy(table_hbm, table_ref, sems.at[1]),
        pltpu.make_async_copy(len_hbm, len_ref, sems.at[2]),
    ]
    for c in copies:
        c.start()
    for c in copies:
        c.wait()
    groups, feats, _ = out_ref.shape
    q = q_ref[...].astype(jnp.float32)
    lane = iota((feats, LANES), 1)
    wide = jnp.concatenate([q, jnp.zeros((2 * feats, 2 * LANES - q.shape[1]), jnp.float32)], axis=1)

    def turned(part, shift):
        shift %= 2 * LANES
        return (part if shift == 0 else pltpu.roll(part, shift, 1))[:, :LANES]

    for g in range(groups):
        low = turned(wide[:feats], -g * TOK)
        high = turned(wide[feats:], HALF - g * TOK)
        both = jnp.where(lane < TOK, low, jnp.where((lane >= HALF) & (lane < HALF + TOK), high, 0.0))
        out_ref[g] = both.astype(out_ref.dtype)

    lane4 = iota((SEQS, LANES), 1)
    sub4 = iota((SEQS, LANES), 0)
    lens = jnp.zeros((SEQS, LANES), jnp.int32)
    for q in range(SEQS):
        lens = jnp.where(sub4 == q, len_ref[0, q], lens)
    local = jnp.where(lane4 < lens, table_ref[...] - first_ref[0], -1)
    row = iota((ROWS, LANES), 0)
    seq = jnp.where(row >= TOK, row - TOK, row) // STEPS
    for s in range(SLOTS):
        hit = jnp.max((local == s).astype(jnp.float32), axis=1, keepdims=True)
        off = jnp.broadcast_to(jnp.where(hit > 0.0, 0.0, EMPTY), (SEQS, LANES))
        b = jnp.broadcast_to(off[0:1], (ROWS, LANES))
        for q in range(1, SEQS):
            b = jnp.where(seq == q, off[q : q + 1], b)
        bias_ref[:, s * BLOCK : (s + 1) * BLOCK] = b


def spread_kernel(a_ref, out_ref):
    feats = a_ref.shape[0]
    row = iota((ROWS, LANES), 0)
    tok = jnp.where(row >= TOK, row - TOK, row)
    lane = iota((ROWS, LANES), 1)
    nt = (((1,), (1,)), ((), ()))
    tiles = [a_ref[g : g + HALF_FEATS] for g in range(0, feats, HALF_FEATS)]
    twice = jnp.concatenate([t for t in tiles for _ in range(2)], axis=0)
    pick = jnp.concatenate([lane == tok, lane == tok + HALF], axis=0).astype(jnp.bfloat16)
    both = lax.dot_general(pick, twice, nt, preferred_element_type=jnp.float32)
    odd = (iota((ROWS, 2 * feats), 1) // HALF_FEATS) % 2 == 1
    whole = jnp.where(odd, both[ROWS:], both[:ROWS])
    rows = jnp.where(row < TOK, whole[:, :LANES], whole[:, LANES:]).astype(out_ref.dtype)
    for b in range(out_ref.shape[0]):
        out_ref[b] = rows


def attend_kernel(bias_ref, q_ref, k_ref, v_ref, out_ref, s_ref, p_ref, top_ref, sum_ref):
    rows = SLICES * ROWS
    lane = iota((rows, LANES), 1)
    lse = jnp.zeros((rows, LANES), jnp.float32)
    nt = (((1,), (1,)), ((), ()))
    nn = (((1,), (0,)), ((), ()))

    def cols(k):
        return slice(k * DH, (k + 1) * DH)

    def scores(k):
        qk = jnp.concatenate([q_ref[STAND[k * SLICES + j]] for j in range(SLICES)], axis=0)
        most = None
        for j in range(0, SLOTS * BLOCK, WIDE):
            at = slice(j, j + WIDE)
            s = lax.dot_general(qk, k_ref[at, cols(k)], nt, preferred_element_type=jnp.float32)
            s = s + jnp.concatenate([bias_ref[:, at]] * SLICES, axis=0)
            s_ref[k % 2, :, at] = s
            for i in range(0, WIDE, LANES):
                part = s[:, i : i + LANES]
                most = part if most is None else jnp.maximum(most, part)
        top = jnp.max(most, axis=1, keepdims=True)
        top_ref[k] = jnp.broadcast_to(top, (rows, LANES))

    def weights(k, lse):
        for r in range(0, rows, CHUNK):
            at = slice(r, r + CHUNK)
            top = top_ref[k, at]
            total = None
            for j in range(0, SLOTS * BLOCK, LANES):
                here = slice(j, j + LANES)
                p = jnp.exp2((s_ref[k % 2, at, here] - top) * SCALE)
                total = p if total is None else total + p
                p_ref[k % 2, at, here] = p.astype(jnp.bfloat16)
            sum_ref[k % 2, at] = jnp.broadcast_to(
                jnp.sum(total, axis=1, keepdims=True), (CHUNK, LANES)
            )
        return jnp.where(lane == k, top_ref[k] * SCALE + jnp.log2(sum_ref[k % 2]), lse)

    def values(k):
        o = lax.dot_general(
            p_ref[k % 2], v_ref[:, cols(k)], nn, preferred_element_type=jnp.float32
        )
        o = (o * (1.0 / sum_ref[k % 2])).astype(out_ref.dtype)
        for j in range(SLICES):
            out_ref[STAND[k * SLICES + j], :ROWS, :] = o[j * ROWS : (j + 1) * ROWS]

    for step in range(KVH + 2):
        if step < KVH:
            scores(step)
        if 0 <= step - 1 < KVH:
            lse = weights(step - 1, lse)
        if step >= 2:
            values(step - 2)
    square = jnp.concatenate([lse, jnp.zeros((LANES - rows, LANES), jnp.float32)], axis=0)
    flat = jnp.transpose(square)[:KVH]
    lane8 = iota((KVH, LANES), 1)
    for j in range(SLICES):
        mine = flat if j == 0 else pltpu.roll(flat, LANES - j * ROWS, 1)
        mine = jnp.where(lane8 < ROWS, mine, 0.0)
        high = mine.astype(jnp.bfloat16).astype(jnp.float32)
        rest = mine - high
        mid = rest.astype(jnp.bfloat16).astype(jnp.float32)
        low = rest - mid
        line = high + pltpu.roll(mid, 32, 1) + pltpu.roll(low, 64, 1)
        for k in range(KVH):
            tile = jnp.broadcast_to(line[k : k + 1], (8, LANES))
            out_ref[STAND[k * SLICES + j], ROWS:, :] = tile.astype(out_ref.dtype)


def combine_kernel(a_ref, out_ref):
    devices = a_ref.shape[0]
    sub8 = iota((8, LANES), 0)
    parts = []
    for t in range(devices // 8):
        acc = a_ref[8 * t, ROWS:, :].astype(jnp.float32)
        for j in range(1, 8):
            acc = jnp.where(sub8 == j, a_ref[8 * t + j, ROWS:, :].astype(jnp.float32), acc)
        parts.append(acc)
    stat = jnp.concatenate(parts, axis=0)
    lse = stat + pltpu.roll(stat, LANES - 32, 1) + pltpu.roll(stat, LANES - 64, 1)
    top = jnp.max(lse, axis=0, keepdims=True)
    w = jnp.exp2(lse - top)
    w = w / jnp.sum(w, axis=0, keepdims=True)
    square = jnp.concatenate([w, jnp.zeros((LANES - devices, LANES), jnp.float32)], axis=0)
    wt = jnp.transpose(square)[:ROWS]
    acc = jnp.zeros((ROWS, LANES), jnp.float32)
    for b in range(devices):
        acc = acc + wt[:, b : b + 1] * a_ref[b, :ROWS, :].astype(jnp.float32)
    out_ref[...] = jnp.concatenate([acc[:TOK], acc[TOK:]], axis=1).astype(out_ref.dtype)


def exchange(pieces):
    return lax.all_to_all(
        pieces, "blk", split_axis=0, concat_axis=0, tiled=True, axis_index_groups=[WALK]
    )


def body(queries, key_pool, value_pool, lengths, block_table):
    bf16 = jnp.bfloat16
    groups = lax.axis_size("grp")
    devices = lax.axis_size("blk")
    first = (lax.axis_index("blk") * SLOTS).astype(jnp.int32).reshape(1)
    packed, bias = pl.pallas_call(
        pack_kernel,
        out_shape=(
            jax.ShapeDtypeStruct((groups, HALF_FEATS, LANES), bf16),
            jax.ShapeDtypeStruct((ROWS, SLOTS * BLOCK), jnp.float32),
        ),
        in_specs=[SMEM, HBM, HBM, HBM],
        out_specs=(VMEM, VMEM),
        scratch_shapes=[
            pltpu.SMEM(lengths.shape, jnp.int32),
            pltpu.VMEM(block_table.shape[1:], jnp.int32),
            pltpu.VMEM(queries.shape[::-1], bf16),
            pltpu.SemaphoreType.DMA((3,)),
        ],
        compiler_params=PARAMS,
        cost_estimate=LONG,
        name="pack",
    )(first, in_hbm(lengths), in_hbm(block_table[0]), in_hbm(queries.T))
    arrived = lax.all_to_all(packed, "grp", split_axis=0, concat_axis=0, tiled=True)
    spread = pl.pallas_call(
        spread_kernel,
        out_shape=jax.ShapeDtypeStruct((devices, ROWS, LANES), bf16),
        in_specs=[VMEM],
        out_specs=VMEM,
        compiler_params=PARAMS,
        cost_estimate=LONG,
        name="spread",
    )(arrived.reshape(groups * HALF_FEATS, LANES))
    query_all = exchange(spread)
    rows = SLICES * ROWS
    pool = (SLOTS * BLOCK, KVH * DH)
    partial = pl.pallas_call(
        attend_kernel,
        out_shape=jax.ShapeDtypeStruct((devices, ROWS + 8, LANES), bf16),
        in_specs=[VMEM] * 4,
        out_specs=VMEM,
        scratch_shapes=[
            pltpu.VMEM((2, rows, pool[0]), jnp.float32),
            pltpu.VMEM((2, rows, pool[0]), bf16),
            pltpu.VMEM((KVH, rows, LANES), jnp.float32),
            pltpu.VMEM((2, rows, LANES), jnp.float32),
        ],
        compiler_params=PARAMS,
        cost_estimate=LONG,
        name="attend",
    )(bias, query_all, key_pool.reshape(pool), value_pool.reshape(pool))
    collected = exchange(partial)
    return pl.pallas_call(
        combine_kernel,
        out_shape=jax.ShapeDtypeStruct((TOK, HEADS * DH), bf16),
        in_specs=[VMEM],
        out_specs=VMEM,
        compiler_params=PARAMS,
        name="combine",
    )(collected)


def solution(mesh):
    placed = (
        P(None, ("blk", "grp")),
        P("grp", "blk", None, None),
        P("grp", "blk", None, None),
        P("grp", None),
        P("grp", None, None),
    )
    return jax.shard_map(
        body, mesh=mesh, in_specs=placed, out_specs=P("grp", "blk"), check_vma=False
    )
```

```python
import math

import jax
import jax.numpy as jnp
from jax import lax
from jax.experimental import pallas as pl
from jax.experimental.pallas import tpu as pltpu
from jax.sharding import PartitionSpec as P

HQ = 64
KVH = 8
DH = 128
STEPS = 3
SEQS = 4
TOK = SEQS * STEPS
HEADS = 2
ROWS = HEADS * TOK
SLICES = 4
SLOTS = 8
WIDE = 256
CHUNK = 16
BLOCK = 128
LANES = 128
HALF_FEATS = 8
HALF = 16
SCALE = math.log2(math.e) / math.sqrt(DH)
LN2 = math.log(2.0)
EMPTY = -1e30

SIDE_X, SIDE_Y = 4, 8
WALK = [
    (x if y % 2 == 0 else SIDE_X - 1 - x) * SIDE_Y + y for y in range(SIDE_Y) for x in range(SIDE_X)
]
STAND = [WALK.index(b) for b in range(len(WALK))]

VMEM = pl.BlockSpec(memory_space=pltpu.VMEM)
HBM = pl.BlockSpec(memory_space=pltpu.HBM)


LONG = pl.CostEstimate(flops=10**10, bytes_accessed=10**8, transcendentals=10**6)
PARAMS = pltpu.CompilerParams(vmem_limit_bytes=16 * 1024 * 1024)


def in_hbm(array):
    return pltpu.with_memory_space_constraint(array, pltpu.HBM)


def iota(shape, dim):
    return lax.broadcasted_iota(jnp.int32, shape, dim)


def pack_kernel(
    len_hbm, table_hbm, q_hbm, out_ref, bias_ref, len_ref, table_ref, q_ref, sems
):
    copies = [
        pltpu.make_async_copy(q_hbm, q_ref, sems.at[0]),
        pltpu.make_async_copy(table_hbm, table_ref, sems.at[1]),
        pltpu.make_async_copy(len_hbm, len_ref, sems.at[2]),
    ]
    for c in copies:
        c.start()
    for c in copies:
        c.wait()
    groups, feats, _ = out_ref.shape
    q = q_ref[...].astype(jnp.float32)
    lane = iota((feats, LANES), 1)
    wide = jnp.concatenate([q, jnp.zeros((2 * feats, 2 * LANES - q.shape[1]), jnp.float32)], axis=1)

    def turned(part, shift):
        shift %= 2 * LANES
        return (part if shift == 0 else pltpu.roll(part, shift, 1))[:, :LANES]

    for g in range(groups):
        low = turned(wide[:feats], -g * TOK)
        high = turned(wide[feats:], HALF - g * TOK)
        both = jnp.where(lane < TOK, low, jnp.where((lane >= HALF) & (lane < HALF + TOK), high, 0.0))
        out_ref[g] = both.astype(out_ref.dtype)

    lane4 = iota((SEQS, LANES), 1)
    sub4 = iota((SEQS, LANES), 0)
    lens = jnp.zeros((SEQS, LANES), jnp.int32)
    for q in range(SEQS):
        lens = jnp.where(sub4 == q, len_ref[0, q], lens)
    local = jnp.where(lane4 < lens, table_ref[...] - lax.axis_index("blk") * SLOTS, -1)
    row = iota((ROWS, LANES), 0)
    seq = jnp.where(row >= TOK, row - TOK, row) // STEPS
    for s in range(SLOTS):
        hit = jnp.max((local == s).astype(jnp.float32), axis=1, keepdims=True)
        off = jnp.broadcast_to(jnp.where(hit > 0.0, 0.0, EMPTY), (SEQS, LANES))
        b = jnp.broadcast_to(off[0:1], (ROWS, LANES))
        for q in range(1, SEQS):
            b = jnp.where(seq == q, off[q : q + 1], b)
        bias_ref[:, s * BLOCK : (s + 1) * BLOCK] = b


def spread_kernel(a_ref, out_ref):
    feats = a_ref.shape[0]
    row = iota((ROWS, LANES), 0)
    tok = jnp.where(row >= TOK, row - TOK, row)
    lane = iota((ROWS, LANES), 1)
    nt = (((1,), (1,)), ((), ()))
    tiles = [a_ref[g : g + HALF_FEATS] for g in range(0, feats, HALF_FEATS)]
    twice = jnp.concatenate([t for t in tiles for _ in range(2)], axis=0)
    pick = jnp.concatenate([lane == tok, lane == tok + HALF], axis=0).astype(jnp.bfloat16)
    both = lax.dot_general(pick, twice, nt, preferred_element_type=jnp.float32)
    odd = (iota((ROWS, 2 * feats), 1) // HALF_FEATS) % 2 == 1
    whole = jnp.where(odd, both[ROWS:], both[:ROWS])
    rows = jnp.where(row < TOK, whole[:, :LANES], whole[:, LANES:]).astype(out_ref.dtype)
    for b in range(out_ref.shape[0]):
        out_ref[b] = rows


def attend_kernel(bias_ref, q_ref, k_ref, v_ref, out_ref, s_ref, p_ref, top_ref, sum_ref):
    rows = SLICES * ROWS
    lane = iota((rows, LANES), 1)
    lse = jnp.zeros((rows, LANES), jnp.float32)
    nt = (((1,), (1,)), ((), ()))
    nn = (((1,), (0,)), ((), ()))

    def cols(k):
        return slice(k * DH, (k + 1) * DH)

    def scores(k):
        qk = jnp.concatenate([q_ref[STAND[k * SLICES + j]] for j in range(SLICES)], axis=0)
        most = None
        for j in range(0, SLOTS * BLOCK, WIDE):
            at = slice(j, j + WIDE)
            s = lax.dot_general(qk, k_ref[at, cols(k)], nt, preferred_element_type=jnp.float32)
            s = s + jnp.concatenate([bias_ref[:, at]] * SLICES, axis=0)
            s_ref[k % 2, :, at] = s
            for i in range(0, WIDE, LANES):
                part = s[:, i : i + LANES]
                most = part if most is None else jnp.maximum(most, part)
        top = jnp.max(most, axis=1, keepdims=True)
        top_ref[k] = jnp.broadcast_to(top, (rows, LANES))

    def weights(k, lse):
        for r in range(0, rows, CHUNK):
            at = slice(r, r + CHUNK)
            top = top_ref[k, at]
            total = None
            for j in range(0, SLOTS * BLOCK, LANES):
                here = slice(j, j + LANES)
                p = jnp.exp2((s_ref[k % 2, at, here] - top) * SCALE)
                total = p if total is None else total + p
                p_ref[k % 2, at, here] = p.astype(jnp.bfloat16)
            sum_ref[k % 2, at] = jnp.broadcast_to(
                jnp.sum(total, axis=1, keepdims=True), (CHUNK, LANES)
            )
        return jnp.where(lane == k, top_ref[k] * SCALE + jnp.log2(sum_ref[k % 2]), lse)

    def values(k):
        o = lax.dot_general(
            p_ref[k % 2], v_ref[:, cols(k)], nn, preferred_element_type=jnp.float32
        )
        o = (o * (1.0 / sum_ref[k % 2])).astype(out_ref.dtype)
        for j in range(SLICES):
            out_ref[STAND[k * SLICES + j], :ROWS, :] = o[j * ROWS : (j + 1) * ROWS]

    for step in range(KVH + 2):
        if step < KVH:
            scores(step)
        if 0 <= step - 1 < KVH:
            lse = weights(step - 1, lse)
        if step >= 2:
            values(step - 2)
    square = jnp.concatenate([lse, jnp.zeros((LANES - rows, LANES), jnp.float32)], axis=0)
    flat = jnp.transpose(square)[:KVH]
    lane8 = iota((KVH, LANES), 1)
    for j in range(SLICES):
        mine = flat if j == 0 else pltpu.roll(flat, LANES - j * ROWS, 1)
        mine = jnp.where(lane8 < ROWS, mine, 0.0)
        high = mine.astype(jnp.bfloat16).astype(jnp.float32)
        rest = mine - high
        mid = rest.astype(jnp.bfloat16).astype(jnp.float32)
        low = rest - mid
        line = high + pltpu.roll(mid, 32, 1) + pltpu.roll(low, 64, 1)
        for k in range(KVH):
            tile = jnp.broadcast_to(line[k : k + 1], (8, LANES))
            out_ref[STAND[k * SLICES + j], ROWS:, :] = tile.astype(out_ref.dtype)


def combine_kernel(a_ref, out_ref):
    devices = a_ref.shape[0]
    sub8 = iota((8, LANES), 0)
    parts = []
    for t in range(devices // 8):
        acc = a_ref[8 * t, ROWS:, :].astype(jnp.float32)
        for j in range(1, 8):
            acc = jnp.where(sub8 == j, a_ref[8 * t + j, ROWS:, :].astype(jnp.float32), acc)
        parts.append(acc)
    stat = jnp.concatenate(parts, axis=0)
    lse = stat + pltpu.roll(stat, LANES - 32, 1) + pltpu.roll(stat, LANES - 64, 1)
    top = jnp.max(lse, axis=0, keepdims=True)
    w = jnp.exp2(lse - top)
    w = w / jnp.sum(w, axis=0, keepdims=True)
    square = jnp.concatenate([w, jnp.zeros((LANES - devices, LANES), jnp.float32)], axis=0)
    wt = jnp.transpose(square)[:ROWS]
    acc = jnp.zeros((ROWS, LANES), jnp.float32)
    for b in range(devices):
        acc = acc + wt[:, b : b + 1] * a_ref[b, :ROWS, :].astype(jnp.float32)
    out_ref[...] = jnp.concatenate([acc[:TOK], acc[TOK:]], axis=1).astype(out_ref.dtype)


def exchange(pieces):
    return lax.all_to_all(
        pieces, "blk", split_axis=0, concat_axis=0, tiled=True, axis_index_groups=[WALK]
    )


def body(queries, key_pool, value_pool, lengths, block_table):
    bf16 = jnp.bfloat16
    groups = lax.axis_size("grp")
    devices = lax.axis_size("blk")
    packed, bias = pl.pallas_call(
        pack_kernel,
        out_shape=(
            jax.ShapeDtypeStruct((groups, HALF_FEATS, LANES), bf16),
            jax.ShapeDtypeStruct((ROWS, SLOTS * BLOCK), jnp.float32),
        ),
        in_specs=[HBM, HBM, HBM],
        out_specs=(VMEM, VMEM),
        scratch_shapes=[
            pltpu.SMEM(lengths.shape, jnp.int32),
            pltpu.VMEM(block_table.shape[1:], jnp.int32),
            pltpu.VMEM(queries.shape[::-1], bf16),
            pltpu.SemaphoreType.DMA((3,)),
        ],
        compiler_params=PARAMS,
        cost_estimate=LONG,
        name="pack",
    )(in_hbm(lengths), in_hbm(block_table[0]), in_hbm(queries.T))
    arrived = lax.all_to_all(packed, "grp", split_axis=0, concat_axis=0, tiled=True)
    spread = pl.pallas_call(
        spread_kernel,
        out_shape=jax.ShapeDtypeStruct((devices, ROWS, LANES), bf16),
        in_specs=[VMEM],
        out_specs=VMEM,
        compiler_params=PARAMS,
        cost_estimate=LONG,
        name="spread",
    )(arrived.reshape(groups * HALF_FEATS, LANES))
    query_all = exchange(spread)
    rows = SLICES * ROWS
    pool = (SLOTS * BLOCK, KVH * DH)
    partial = pl.pallas_call(
        attend_kernel,
        out_shape=jax.ShapeDtypeStruct((devices, ROWS + 8, LANES), bf16),
        in_specs=[VMEM] * 4,
        out_specs=VMEM,
        scratch_shapes=[
            pltpu.VMEM((2, rows, pool[0]), jnp.float32),
            pltpu.VMEM((2, rows, pool[0]), bf16),
            pltpu.VMEM((KVH, rows, LANES), jnp.float32),
            pltpu.VMEM((2, rows, LANES), jnp.float32),
        ],
        compiler_params=PARAMS,
        cost_estimate=LONG,
        name="attend",
    )(bias, query_all, key_pool.reshape(pool), value_pool.reshape(pool))
    collected = exchange(partial)
    return pl.pallas_call(
        combine_kernel,
        out_shape=jax.ShapeDtypeStruct((TOK, HEADS * DH), bf16),
        in_specs=[VMEM],
        out_specs=VMEM,
        compiler_params=PARAMS,
        name="combine",
    )(collected)


def solution(mesh):
    placed = (
        P(None, ("blk", "grp")),
        P("grp", "blk", None, None),
        P("grp", "blk", None, None),
        P("grp", None),
        P("grp", None, None),
    )
    return jax.shard_map(
        body, mesh=mesh, in_specs=placed, out_specs=P("grp", "blk"), check_vma=False
    )
```

```python
import math

import jax
import jax.numpy as jnp
from jax import lax
from jax.experimental import pallas as pl
from jax.experimental.pallas import tpu as pltpu
from jax.sharding import PartitionSpec as P

HQ = 64
KVH = 8
DH = 128
STEPS = 3
SEQS = 4
TOK = SEQS * STEPS
HEADS = 2
ROWS = HEADS * TOK
SLICES = 4
SLOTS = 8
WIDE = 256
CHUNK = 16
BLOCK = 128
LANES = 128
HALF_FEATS = 8
HALF = 16
SCALE = math.log2(math.e) / math.sqrt(DH)
LN2 = math.log(2.0)
EMPTY = -1e30

SIDE_X, SIDE_Y = 4, 8
WALK = [
    (x if y % 2 == 0 else SIDE_X - 1 - x) * SIDE_Y + y for y in range(SIDE_Y) for x in range(SIDE_X)
]
STAND = [WALK.index(b) for b in range(len(WALK))]

VMEM = pl.BlockSpec(memory_space=pltpu.VMEM)
HBM = pl.BlockSpec(memory_space=pltpu.HBM)
SMEM = pl.BlockSpec(memory_space=pltpu.SMEM)


LONG = pl.CostEstimate(flops=10**10, bytes_accessed=10**8, transcendentals=10**6)
PARAMS = pltpu.CompilerParams(vmem_limit_bytes=16 * 1024 * 1024)


def in_hbm(array):
    return pltpu.with_memory_space_constraint(array, pltpu.HBM)


def iota(shape, dim):
    return lax.broadcasted_iota(jnp.int32, shape, dim)


def pack_kernel(
    first_ref, len_hbm, table_hbm, q_hbm, out_ref, bias_ref, len_ref, table_ref, q_ref, sems
):
    copies = [
        pltpu.make_async_copy(q_hbm, q_ref, sems.at[0]),
        pltpu.make_async_copy(table_hbm, table_ref, sems.at[1]),
        pltpu.make_async_copy(len_hbm, len_ref, sems.at[2]),
    ]
    for c in copies:
        c.start()
    for c in copies:
        c.wait()
    groups, feats, _ = out_ref.shape
    q = q_ref[...].astype(jnp.float32)
    lane = iota((feats, LANES), 1)
    wide = jnp.concatenate([q, jnp.zeros((2 * feats, 2 * LANES - q.shape[1]), jnp.float32)], axis=1)

    def turned(part, shift):
        shift %= 2 * LANES
        return (part if shift == 0 else pltpu.roll(part, shift, 1))[:, :LANES]

    for g in range(groups):
        low = turned(wide[:feats], -g * TOK)
        high = turned(wide[feats:], HALF - g * TOK)
        both = jnp.where(lane < TOK, low, jnp.where((lane >= HALF) & (lane < HALF + TOK), high, 0.0))
        out_ref[g] = both.astype(out_ref.dtype)

    lane4 = iota((SEQS, LANES), 1)
    sub4 = iota((SEQS, LANES), 0)
    lens = jnp.zeros((SEQS, LANES), jnp.int32)
    for q in range(SEQS):
        lens = jnp.where(sub4 == q, len_ref[0, q], lens)
    local = jnp.where(lane4 < lens, table_ref[...] - first_ref[0], -1)
    row = iota((ROWS, LANES), 0)
    seq = jnp.where(row >= TOK, row - TOK, row) // STEPS
    for s in range(SLOTS):
        hit = jnp.max((local == s).astype(jnp.float32), axis=1, keepdims=True)
        off = jnp.broadcast_to(jnp.where(hit > 0.0, 0.0, EMPTY), (SEQS, LANES))
        b = jnp.broadcast_to(off[0:1], (ROWS, LANES))
        for q in range(1, SEQS):
            b = jnp.where(seq == q, off[q : q + 1], b)
        bias_ref[:, s * BLOCK : (s + 1) * BLOCK] = b


def spread_kernel(a_ref, out_ref):
    feats = a_ref.shape[0]
    row = iota((ROWS, LANES), 0)
    tok = jnp.where(row >= TOK, row - TOK, row)
    lane = iota((ROWS, LANES), 1)
    nt = (((1,), (1,)), ((), ()))
    tiles = [a_ref[g : g + HALF_FEATS] for g in range(0, feats, HALF_FEATS)]
    twice = jnp.concatenate([t for t in tiles for _ in range(2)], axis=0)
    pick = jnp.concatenate([lane == tok, lane == tok + HALF], axis=0).astype(jnp.bfloat16)
    both = lax.dot_general(pick, twice, nt, preferred_element_type=jnp.float32)
    odd = (iota((ROWS, 2 * feats), 1) // HALF_FEATS) % 2 == 1
    whole = jnp.where(odd, both[ROWS:], both[:ROWS])
    rows = jnp.where(row < TOK, whole[:, :LANES], whole[:, LANES:]).astype(out_ref.dtype)
    for b in range(out_ref.shape[0]):
        out_ref[b] = rows


def attend_kernel(bias_ref, q_ref, k_ref, v_ref, out_ref, s_ref, p_ref, top_ref, sum_ref):
    rows = SLICES * ROWS
    lane = iota((rows, LANES), 1)
    lse = jnp.zeros((rows, LANES), jnp.float32)
    nt = (((1,), (1,)), ((), ()))
    nn = (((1,), (0,)), ((), ()))

    def cols(k):
        return slice(k * DH, (k + 1) * DH)

    def scores(k):
        qk = q_ref[k * SLICES : (k + 1) * SLICES].reshape(rows, DH)
        most = None
        for j in range(0, SLOTS * BLOCK, WIDE):
            at = slice(j, j + WIDE)
            s = lax.dot_general(qk, k_ref[at, cols(k)], nt, preferred_element_type=jnp.float32)
            s = s + jnp.concatenate([bias_ref[:, at]] * SLICES, axis=0)
            s_ref[k % 2, :, at] = s
            for i in range(0, WIDE, LANES):
                part = s[:, i : i + LANES]
                most = part if most is None else jnp.maximum(most, part)
        top = jnp.max(most, axis=1, keepdims=True)
        top_ref[k] = jnp.broadcast_to(top, (rows, LANES))

    def weights(k, lse):
        for r in range(0, rows, CHUNK):
            at = slice(r, r + CHUNK)
            top = top_ref[k, at]
            total = None
            for j in range(0, SLOTS * BLOCK, LANES):
                here = slice(j, j + LANES)
                p = jnp.exp2((s_ref[k % 2, at, here] - top) * SCALE)
                total = p if total is None else total + p
                p_ref[k % 2, at, here] = p.astype(jnp.bfloat16)
            sum_ref[k % 2, at] = jnp.broadcast_to(
                jnp.sum(total, axis=1, keepdims=True), (CHUNK, LANES)
            )
        return jnp.where(lane == k, top_ref[k] * SCALE + jnp.log2(sum_ref[k % 2]), lse)

    def values(k):
        o = lax.dot_general(
            p_ref[k % 2], v_ref[:, cols(k)], nn, preferred_element_type=jnp.float32
        )
        o = (o * (1.0 / sum_ref[k % 2])).astype(out_ref.dtype)
        for j in range(SLICES):
            out_ref[STAND[k * SLICES + j], :ROWS, :] = o[j * ROWS : (j + 1) * ROWS]

    for step in range(KVH + 2):
        if step < KVH:
            scores(step)
        if 0 <= step - 1 < KVH:
            lse = weights(step - 1, lse)
        if step >= 2:
            values(step - 2)
    square = jnp.concatenate([lse, jnp.zeros((LANES - rows, LANES), jnp.float32)], axis=0)
    flat = jnp.transpose(square)[:KVH]
    lane8 = iota((KVH, LANES), 1)
    for j in range(SLICES):
        mine = flat if j == 0 else pltpu.roll(flat, LANES - j * ROWS, 1)
        mine = jnp.where(lane8 < ROWS, mine, 0.0)
        high = mine.astype(jnp.bfloat16).astype(jnp.float32)
        rest = mine - high
        mid = rest.astype(jnp.bfloat16).astype(jnp.float32)
        low = rest - mid
        line = high + pltpu.roll(mid, 32, 1) + pltpu.roll(low, 64, 1)
        for k in range(KVH):
            tile = jnp.broadcast_to(line[k : k + 1], (8, LANES))
            out_ref[STAND[k * SLICES + j], ROWS:, :] = tile.astype(out_ref.dtype)


def combine_kernel(a_ref, out_ref):
    devices = a_ref.shape[0]
    sub8 = iota((8, LANES), 0)
    parts = []
    for t in range(devices // 8):
        acc = a_ref[8 * t, ROWS:, :].astype(jnp.float32)
        for j in range(1, 8):
            acc = jnp.where(sub8 == j, a_ref[8 * t + j, ROWS:, :].astype(jnp.float32), acc)
        parts.append(acc)
    stat = jnp.concatenate(parts, axis=0)
    lse = stat + pltpu.roll(stat, LANES - 32, 1) + pltpu.roll(stat, LANES - 64, 1)
    top = jnp.max(lse, axis=0, keepdims=True)
    w = jnp.exp2(lse - top)
    w = w / jnp.sum(w, axis=0, keepdims=True)
    square = jnp.concatenate([w, jnp.zeros((LANES - devices, LANES), jnp.float32)], axis=0)
    wt = jnp.transpose(square)[:ROWS]
    acc = jnp.zeros((ROWS, LANES), jnp.float32)
    for b in range(devices):
        acc = acc + wt[:, b : b + 1] * a_ref[b, :ROWS, :].astype(jnp.float32)
    out_ref[...] = jnp.concatenate([acc[:TOK], acc[TOK:]], axis=1).astype(out_ref.dtype)


def exchange(pieces):
    return lax.all_to_all(
        pieces, "blk", split_axis=0, concat_axis=0, tiled=True, axis_index_groups=[WALK]
    )


def body(queries, key_pool, value_pool, lengths, block_table):
    bf16 = jnp.bfloat16
    groups = lax.axis_size("grp")
    devices = lax.axis_size("blk")
    first = (lax.axis_index("blk") * SLOTS).astype(jnp.int32).reshape(1)
    packed, bias = pl.pallas_call(
        pack_kernel,
        out_shape=(
            jax.ShapeDtypeStruct((groups, HALF_FEATS, LANES), bf16),
            jax.ShapeDtypeStruct((ROWS, SLOTS * BLOCK), jnp.float32),
        ),
        in_specs=[SMEM, HBM, HBM, HBM],
        out_specs=(VMEM, VMEM),
        scratch_shapes=[
            pltpu.SMEM(lengths.shape, jnp.int32),
            pltpu.VMEM(block_table.shape[1:], jnp.int32),
            pltpu.VMEM(queries.shape[::-1], bf16),
            pltpu.SemaphoreType.DMA((3,)),
        ],
        compiler_params=PARAMS,
        cost_estimate=LONG,
        name="pack",
    )(first, in_hbm(lengths), in_hbm(block_table[0]), in_hbm(queries.T))
    arrived = lax.all_to_all(packed, "grp", split_axis=0, concat_axis=0, tiled=True)
    spread = pl.pallas_call(
        spread_kernel,
        out_shape=jax.ShapeDtypeStruct((devices, ROWS, LANES), bf16),
        in_specs=[VMEM],
        out_specs=VMEM,
        compiler_params=PARAMS,
        cost_estimate=LONG,
        name="spread",
    )(arrived.reshape(groups * HALF_FEATS, LANES))
    query_all = lax.all_to_all(spread, "blk", split_axis=0, concat_axis=0, tiled=True)
    rows = SLICES * ROWS
    pool = (SLOTS * BLOCK, KVH * DH)
    partial = pl.pallas_call(
        attend_kernel,
        out_shape=jax.ShapeDtypeStruct((devices, ROWS + 8, LANES), bf16),
        in_specs=[VMEM] * 4,
        out_specs=VMEM,
        scratch_shapes=[
            pltpu.VMEM((2, rows, pool[0]), jnp.float32),
            pltpu.VMEM((2, rows, pool[0]), bf16),
            pltpu.VMEM((KVH, rows, LANES), jnp.float32),
            pltpu.VMEM((2, rows, LANES), jnp.float32),
        ],
        compiler_params=PARAMS,
        cost_estimate=LONG,
        name="attend",
    )(bias, query_all, key_pool.reshape(pool), value_pool.reshape(pool))
    collected = exchange(partial)
    return pl.pallas_call(
        combine_kernel,
        out_shape=jax.ShapeDtypeStruct((TOK, HEADS * DH), bf16),
        in_specs=[VMEM],
        out_specs=VMEM,
        compiler_params=PARAMS,
        name="combine",
    )(collected)


def solution(mesh):
    placed = (
        P(None, ("blk", "grp")),
        P("grp", "blk", None, None),
        P("grp", "blk", None, None),
        P("grp", None),
        P("grp", None, None),
    )
    return jax.shard_map(
        body, mesh=mesh, in_specs=placed, out_specs=P("grp", "blk"), check_vma=False
    )
```
